256 devices in a mesh: seq: 64 (over x, z, y_hi), tp: 4 (over y_lo, core).
Axes of the slice: x: 4, y: 4 (y_hi: 2, y_lo: 2; y = y_hi * 2 + y_lo), z: 8, core: 2. Of those that a mesh axis runs over, the one named last changes fastest.
Arguments:
- queries: bfloat16 [12288, 4096], P('seq', 'tp'), may hold values from -80 to 80
- keys: bfloat16 [12288, 512], P('seq', 'tp'), may hold values from -4 to 4
- values: bfloat16 [12288, 512], P('seq', 'tp'), may hold values from -6 to 6
- segment_ids: int32 [12288], P('seq'), may hold values from 0 to 15, never falling along the last dimension, each value on 1 to 9216 neighbouring positions
- out_weight: bfloat16 [4096, 8192], P('tp', 'seq'), may hold values from -0.09375 to 0.09375
Outputs:
- projected: bfloat16 [12288, 8192], P('seq', 'tp')
The draws below stay inside these ranges and needn't reach their ends.
Inputs may be any that keep to these rules, and one draw needn't show every extreme that they name: `segment_ids`: segment numbers never fall along the sequence and every number from 0 to 15 occurs; no document has more than 9216 tokens and one has exactly that many.
All inputs are finite; a program needn't handle non-finite values.
Results may differ from the reference program's by a relative error of at most 0.012.
Values may be sent and summed in bfloat16 or wider, within the bound.
A program may use at most 128 MiB of HBM per device.

```python
import math
import jax
import jax.numpy as jnp
import numpy as np
from jax import lax

HEADS = 32
KV_HEADS = 4
HEAD_DIM = 128
OUT_WIDTH = 8192
SEGMENTS = 16
TOKENS = 12288
N_TP = 4


def draw_key_field(key):
    base_draw = jax.random.normal(jax.random.fold_in(key, 11), (TOKENS, KV_HEADS * HEAD_DIM), jnp.float32)
    return jnp.clip(base_draw, -4.0, 4.0)


def draw_keys(key, part):
    return draw_key_field(key).astype(jnp.bfloat16)


def draw_queries(key, part):
    fresh_draw = 3.0 * jnp.clip(jax.random.normal(jax.random.fold_in(key, 12), (TOKENS, HEADS * HEAD_DIM), jnp.float32), -6.0, 6.0)
    return fresh_draw.astype(jnp.bfloat16)


def levels(stream_key, dims, pieces, low, top_value):
    level, own = 1.0, jax.random.fold_in(stream_key, 6)
    for dim, parts in pieces:
        heights = jnp.exp(jax.random.uniform(jax.random.fold_in(own, dim), (parts,), jnp.float32, low / len(pieces), top_value / len(pieces)))
        level = level * jnp.repeat(heights, dims[dim] // parts).reshape([-1 if axis == dim else 1 for axis in range(len(dims))])
    return level


def length_profile(amount, total, most, skew):
    loads = [(1 << 20) // math.isqrt(grade ** skew) + 1 for grade in range(2, amount + 1)]
    spare, given = total - most - (amount - 1), [1] * (amount - 1)
    while spare > 0:
        free = [i for i in range(amount - 1) if given[i] < most]
        whole, remaining = sum([loads[i] for i in free]), spare
        for i in free:
            extra = min(most - given[i], max(1, remaining * loads[i] // whole), spare)
            given[i] = given[i] + extra
            spare = spare - extra
    return np.array([most] + given)


def uneven(own_key, amount, total, reach, lean):
    if amount == 2:
        one = jax.random.randint(own_key, (), max(1, total - reach), min(reach, total - 1) + 1)
        return jnp.stack([one, total - one])
    sizes = jnp.asarray(length_profile(amount, total, reach, lean), jnp.int32)
    twos = (amount - 1) // 2
    donor, taker = sizes[1:1 + 2 * twos:2], sizes[2:2 + 2 * twos:2]
    slack = jnp.minimum(donor - 1, reach - taker)
    shifted = jax.random.randint(jax.random.fold_in(own_key, 1), (twos,), 0, 1 << 20) % (slack + 1)
    sizes = sizes.at[1:1 + 2 * twos:2].set(donor - shifted).at[2:2 + 2 * twos:2].set(taker + shifted)
    return sizes[jax.random.permutation(jax.random.fold_in(own_key, 2), amount)]


def centred(stream_key, extent, width, most, split=(), kind=jnp.bfloat16):
    result = jax.random.normal(stream_key, extent, jnp.float32) * width
    if len(split) > 0:
        result = levels(stream_key, extent, split, -0.22, 0.18) * result
    return jnp.clip(result, min=-most, max=most).astype(kind)


def setup_inputs(seed: int = 0) -> dict:
    splits = jax.random.split(jax.random.key(seed), 6)
    return {
        "queries": draw_queries(jax.random.fold_in(splits[5], 71), 0),
        "keys": draw_keys(jax.random.fold_in(splits[5], 71), 0),
        "values": centred(splits[2], (TOKENS, KV_HEADS * HEAD_DIM), 1.0, 6.0, ((0, 64), (1, 4))),
        "segment_ids": jnp.searchsorted(jnp.cumsum(uneven(splits[3], SEGMENTS, TOKENS, 3 * TOKENS // 4, 2)), jnp.arange(TOKENS), side="right").astype(jnp.int32),
        "out_weight": centred(splits[4], (HEADS * HEAD_DIM, OUT_WIDTH), (HEADS * HEAD_DIM) ** -0.5, 0.09375, ((0, 4), (1, 64))),
    }


rope_base = 500000.0
masked_score = -1e+30

def rotate_heads(inputs, positions, head_dim):
    row_count = inputs.shape[0]
    head_count = inputs.shape[1] // head_dim
    half_dim = head_dim // 2
    widened = inputs.astype(jnp.float32).reshape(row_count, head_count, head_dim)
    exponent = jnp.arange(half_dim, dtype=jnp.float32) * (2.0 / head_dim)
    inverse = jnp.power(jnp.float32(rope_base), -exponent)
    angles = positions.astype(jnp.float32)[:, None] * inverse[None, :]
    cosine_table = jnp.cos(angles)[:, None, :]
    sine_table = jnp.sin(angles)[:, None, :]
    first_half = widened[:, :, :half_dim]
    second_half = widened[:, :, half_dim:]
    turned = jnp.concatenate([first_half * cosine_table - second_half * sine_table, second_half * cosine_table + first_half * sine_table], axis=2)
    return turned.reshape(row_count, head_count * head_dim).astype(jnp.bfloat16)

def doc_counts_of(segment_ids, segments):
    labels = jnp.arange(segments, dtype=jnp.int32)
    return lax.optimization_barrier(jnp.sum((segment_ids[None, :] == labels[:, None]).astype(jnp.int32), axis=1))

def first_rows(segment, starts):
    labels = jnp.arange(starts.shape[0], dtype=jnp.int32)
    return lax.optimization_barrier(jnp.sum(jnp.where(segment[:, None] == labels[None, :], starts[None, :], 0), axis=1)).astype(jnp.int32)

def reference(queries, keys, values, segment_ids, out_weight):
    counts = doc_counts_of(segment_ids, SEGMENTS)
    doc_ends = jnp.cumsum(counts).astype(jnp.int32)
    starts = doc_ends - counts
    every_row = jnp.arange(TOKENS, dtype=jnp.int32)
    positions = every_row - first_rows(segment_ids, starts)
    query_rot = rotate_heads(queries, positions, HEAD_DIM)
    key_rot = rotate_heads(keys, positions, HEAD_DIM)
    group_size = HEADS // KV_HEADS
    score_scale = 1.0 / math.sqrt(HEAD_DIM)
    key_full = lax.optimization_barrier(key_rot).astype(jnp.float32).reshape(TOKENS, KV_HEADS, HEAD_DIM)
    value_full = values.astype(jnp.float32).reshape(TOKENS, KV_HEADS, HEAD_DIM)
    query_block = 128 if TOKENS % 128 == 0 else TOKENS

    def attend(block_number):
        first_row = block_number * query_block
        query_tile = lax.dynamic_slice_in_dim(query_rot, first_row, query_block, 0)
        query_tile = lax.optimization_barrier(query_tile).astype(jnp.float32).reshape(query_block, KV_HEADS, group_size, HEAD_DIM)
        query_rows = first_row + jnp.arange(query_block, dtype=jnp.int32)
        query_segs = lax.dynamic_slice_in_dim(segment_ids, first_row, query_block, 0)
        scores = jnp.einsum('tkgd,skd->kgts', query_tile, key_full, precision=lax.Precision.HIGHEST) * score_scale
        visible = (every_row[None, :] <= query_rows[:, None]) & (segment_ids[None, :] == query_segs[:, None])
        scores = jnp.where(visible[None, None], scores, masked_score)
        row_max = lax.optimization_barrier(jnp.max(scores, axis=-1, keepdims=True))
        weights_full = jnp.where(visible[None, None], jnp.exp(scores - row_max), 0.0)
        normalizer = lax.optimization_barrier(jnp.sum(weights_full, axis=-1))
        weights_low = lax.optimization_barrier(weights_full.astype(jnp.bfloat16)).astype(jnp.float32)
        numerator = jnp.einsum('kgts,skd->kgtd', weights_low, value_full, precision=lax.Precision.HIGHEST)
        output = numerator / normalizer[..., None]
        return jnp.transpose(output, (2, 0, 1, 3)).reshape(query_block, HEADS * HEAD_DIM).astype(jnp.bfloat16)
    attended = lax.map(attend, jnp.arange(TOKENS // query_block, dtype=jnp.int32)).reshape(TOKENS, HEADS * HEAD_DIM)
    head_width = HEADS * HEAD_DIM // N_TP
    summed = jnp.zeros((TOKENS, OUT_WIDTH), jnp.float32)
    for shard in range(N_TP):
        term = jnp.dot(attended[:, shard * head_width:(shard + 1) * head_width], out_weight[shard * head_width:(shard + 1) * head_width], preferred_element_type=jnp.float32).astype(jnp.bfloat16)
        summed = summed + lax.optimization_barrier(term).astype(jnp.float32)
    return summed.astype(jnp.bfloat16)
```

```python
import functools
import math

import jax
import jax.numpy as jnp
from jax import lax
from jax.experimental import pallas as pl
from jax.experimental.pallas import tpu as pltpu
from jax.sharding import PartitionSpec as P

HEAD_DIM = 128
SEGMENTS = 16
NX, NZ = 4, 8
BLK = 192
HALF = 96
GROUP = 8
CHUNK = 384
NCHUNK = 32
WROWS = 1024
WSPLIT = 608
ROPE_BASE = 500000.0
BIG = -1e30
MESH = pl.DeviceIdType.MESH


def coords(j, k):
    return j // 16, (j // 2) % 8, j % 2, k // 2, k % 2


def seq_tp(x, z, h, yl, c):
    return x * 16 + z * 2 + h, yl * 2 + c


def route(fn):
    pairs = []
    for j in range(64):
        for k in range(4):
            dj, dk = fn(j, k)
            pairs.append((j * 4 + k, dj * 4 + dk))
    return pairs


def swap_to(j, k):
    x, z, h, yl, c = coords(j, k)
    return seq_tp(x, z, c, yl, h)


def flip_swap_to(j, k):
    x, z, h, yl, c = coords(j, k)
    return seq_tp(NX - 1 - x, NZ - 1 - z, c, yl, h)


def weight_to(j, k):
    x, z, h, yl, c = coords(j, k)
    return seq_tp(2 * yl + c, z, x % 2, x // 2, h)


def here():
    j = lax.axis_index("seq")
    k = lax.axis_index("tp")
    return coords(j, k)


def ident(x, z, h, yl, c):
    return {"seq": x * 16 + z * 2 + h, "tp": yl * 2 + c}


def mod(value, n):
    return lax.rem(value + 2 * n, n)


def counts_kernel(own_ref, out_ref, part, got, send_sem, recv_sem):
    x, z, h, yl, c = here()
    peers_h = [ident(x, z, 1 - h, yl, c)]
    peers_x = [ident(mod(x + d, NX), z, h, yl, c) for d in range(1, NX)]
    peers_z = [ident(x, mod(z + d, NZ), h, yl, c) for d in range(1, NZ)]
    barrier = pltpu.get_barrier_semaphore()
    for peer in peers_h + peers_x + peers_z:
        pl.semaphore_signal(barrier, inc=1, device_id=peer, device_id_type=MESH)
    pl.semaphore_wait(barrier, 11)
    at = 0
    for phase, peers in enumerate((peers_h, peers_x, peers_z)):
        source = own_ref if phase == 0 else part.at[phase - 1]
        copies = []
        for i, peer in enumerate(peers):
            copy = pltpu.make_async_remote_copy(
                src_ref=source, dst_ref=got.at[at + i], send_sem=send_sem.at[at + i],
                recv_sem=recv_sem.at[at + i], device_id=peer, device_id_type=MESH,
            )
            copy.start()
            copies.append(copy)
        total = source[...]
        for i, copy in enumerate(copies):
            copy.wait()
            total = total + got[at + i]
        at += len(peers)
        if phase < 2:
            part[phase] = total
        else:
            out_ref[...] = total


def counts_total(own):
    return pl.pallas_call(
        counts_kernel,
        out_shape=jax.ShapeDtypeStruct((8, 128), jnp.int32),
        in_specs=[pl.BlockSpec(memory_space=pltpu.VMEM)],
        out_specs=pl.BlockSpec(memory_space=pltpu.VMEM),
        scratch_shapes=[
            pltpu.VMEM((2, 8, 128), jnp.int32),
            pltpu.VMEM((11, 8, 128), jnp.int32),
            pltpu.SemaphoreType.DMA((11,)),
            pltpu.SemaphoreType.DMA((11,)),
        ],
        compiler_params=pltpu.CompilerParams(collective_id=1, has_side_effects=True),
        name="counts",
    )(own)


class Gather:
    def __init__(self, slot, first_axis, place, own, ring_sem, side_sem, send_sem):
        self.slot, self.first_axis, self.place, self.own = slot, first_axis, place, own
        self.ring_sem, self.side_sem, self.send_sem = ring_sem, side_sem, send_sem
        self.sent = []
        self.x, self.z, self.h, self.yl, self.c = here()

    def chunk(self, dx, dz):
        return mod(self.x + dx, NX) * NZ + mod(self.z + dz, NZ)

    def neighbour(self, axis, step):
        if axis == "x":
            return ident(mod(self.x + step, NX), self.z, self.h, self.yl, self.c)
        return ident(self.x, mod(self.z + step, NZ), self.h, self.yl, self.c)

    def send(self, dx, dz, axis, step):
        ci = self.chunk(dx, dz)
        there = self.place(ci, self.c)
        source = self.own if (dx, dz) == (0, 0) else there
        n = len(self.sent)
        if axis == "side":
            target, recv = ident(self.x, self.z, self.h, self.yl, 1 - self.c), self.side_sem.at[self.slot, ci]
        else:
            target, recv = self.neighbour(axis, step), self.ring_sem.at[self.slot, ci]
        copy = pltpu.make_async_remote_copy(
            src_ref=source, dst_ref=there, send_sem=self.send_sem.at[self.slot, n], recv_sem=recv,
            device_id=target, device_id_type=MESH,
        )
        copy.start()
        self.sent.append(copy)

    def arrived(self, dx, dz, side=False):
        ci = self.chunk(dx, dz)
        sem = self.side_sem if side else self.ring_sem
        ref = self.place(ci, 1 - self.c if side else self.c)
        pltpu.make_async_remote_copy(
            src_ref=ref, dst_ref=ref, send_sem=self.send_sem.at[self.slot, 0], recv_sem=sem.at[self.slot, ci],
            device_id=ident(self.x, self.z, self.h, self.yl, 1 - self.c), device_id_type=MESH,
        ).wait_recv()

    def begin(self):
        last = "x" if self.first_axis == "z" else "z"
        for axis in (self.first_axis, last):
            for step in (1, -1):
                self.send(0, 0, axis, step)
        self.send(0, 0, "side", 0)

    def events(self):
        found = []
        if self.first_axis == "z":
            order = []
            for s in range(1, 5):
                found.append((s, 0, -s, ([("z", 1)] if s <= 3 else []) + [("x", 1), ("x", -1)]))
                if s <= 3:
                    found.append((s, 0, s, ([("z", -1)] if s <= 2 else []) + [("x", 1), ("x", -1)]))
            order = [0, -1, 1, -2, 2, -3, 3, -4]
            for i, dz in enumerate(order):
                first = dz % 8 < 4
                found.append((1.5 + 1.5 * i, -1, dz, [("x", 1)] if first else []))
                found.append((1.5 + 1.5 * i, 1, dz, [] if first else [("x", -1)]))
                found.append((4 + 1.5 * i, 2, dz, []))
        else:
            found.append((1, -1, 0, [("x", 1), ("z", 1), ("z", -1)]))
            found.append((1, 1, 0, [("z", 1), ("z", -1)]))
            found.append((2, 2, 0, [("z", 1), ("z", -1)]))
            for s in range(1, 5):
                for i, dx in enumerate((0, -1, 1, 2)):
                    first = dx in (0, 1)
                    when = 1 + 4 * (s - 1) + i
                    if s < 4 or first:
                        onward = s <= 2 or (s == 3 and first)
                        found.append((when, dx, -s, [("z", 1)] if onward else []))
                    if s < 4 or not first:
                        onward = s <= 2 or (s == 3 and not first)
                        found.append((when, dx, s, [("z", -1)] if onward else []))
        return [(t, self, dx, dz % 8 if dz == -4 else dz, sends) for t, dx, dz, sends in found]

    def run(self, dx, dz, sends):
        self.arrived(dx, dz)
        for axis, step in sends:
            self.send(dx, dz, axis, step)
        self.send(dx, dz, "side", 0)

    def finish_sides(self):
        for dx in range(NX):
            for dz in range(NZ):
                self.arrived(dx, dz, side=True)

    def finish_sends(self):
        for copy in self.sent:
            copy.wait_send()


def merged(*gathers):
    return sorted([e for g in gathers for e in g.events()], key=lambda e: e[0])


def main_kernel(
    q_ref, pen_ref, k_ref, v_ref, bound_ref, w_ref, out_ref,
    kall, vall, tags, wall, qa, top, norm, acc, acts, back, backin,
    ring_sem, side_sem, send_sem, act_send, act_recv,
):
    x, z, h, yl, c = here()
    y = 2 * h + yl
    ci = x * NZ + z
    side = ident(x, z, h, yl, 1 - c)
    flip = ident(NX - 1 - x, NZ - 1 - z, h, yl, c)

    def along_y(step):
        there = mod(y + step, 4)
        return ident(x, z, there // 2, lax.rem(there, 2), c)

    def heads_at(step):
        there = mod(y + step, 4)
        return 2 * lax.rem(there, 2) + there // 2

    peers = [
        ident(mod(x + 1, NX), z, h, yl, c), ident(mod(x - 1, NX), z, h, yl, c),
        ident(x, mod(z + 1, NZ), h, yl, c), ident(x, mod(z - 1, NZ), h, yl, c),
        along_y(1), along_y(-1), side, flip,
    ]
    barrier = pltpu.get_barrier_semaphore()
    for peer in peers:
        pl.semaphore_signal(barrier, inc=1, device_id=peer, device_id_type=MESH)
    pl.semaphore_wait(barrier, len(peers))

    sems = (ring_sem, side_sem, send_sem)
    vg = Gather(0, "z", lambda i, t: vall.at[i, t], v_ref, *sems)
    kg = Gather(1, "x", lambda i, t: kall.at[i, t], k_ref, *sems)
    wa = Gather(2, "z", lambda i, t: wall.at[i, t, pl.ds(0, WSPLIT)], w_ref.at[pl.ds(0, WSPLIT)], *sems)
    wb = Gather(3, "x", lambda i, t: wall.at[i, t, pl.ds(WSPLIT, WROWS - WSPLIT)],
                w_ref.at[pl.ds(WSPLIT, WROWS - WSPLIT)], *sems)
    vg.begin()
    kg.begin()
    kall[ci, c] = k_ref[...]
    vall[ci, c] = v_ref[...]
    wall[ci, c] = w_ref[...]
    for half in range(2):
        rows = pl.ds(half * HALF, HALF)
        for head in range(GROUP):
            at = pl.ds(head * HALF, HALF)
            qa[half, at, 0:HEAD_DIM] = q_ref[rows, head * HEAD_DIM : (head + 1) * HEAD_DIM]
            qa[half, at, HEAD_DIM : 2 * HEAD_DIM] = pen_ref[rows, :]

    def tag(i, carry):
        rows = i * CHUNK + lax.broadcasted_iota(jnp.int32, (CHUNK, 128), 0)
        inside = (rows >= bound_ref[0:1, :]) & (rows < bound_ref[1:2, :])
        tags[i] = jnp.where(inside, 1.0, 0.0).astype(jnp.bfloat16)
        return carry

    lax.fori_loop(0, NCHUNK, tag, 0)

    for _, g, dx, dz, sends in merged(vg, kg):
        g.run(dx, dz, sends)
    wa.begin()
    wb.begin()
    vg.finish_sides()
    kg.finish_sides()

    factor = math.log2(math.e) / math.sqrt(HEAD_DIM)

    def scores_of(half, chunk):
        keys = jnp.concatenate([kall[chunk].reshape(CHUNK, HEAD_DIM), tags[chunk]], axis=1)
        return lax.dot_general(qa[half], keys, (((1,), (1,)), ((), ())), preferred_element_type=jnp.float32)

    def times_values(weights, chunk):
        return jnp.dot(
            weights.astype(jnp.bfloat16), vall[chunk].reshape(CHUNK, HEAD_DIM), preferred_element_type=jnp.float32
        )

    def diagonal(half, chunk, first):
        scores = scores_of(half, chunk)
        row = lax.rem(lax.broadcasted_iota(jnp.int32, scores.shape, 0), HALF) + first
        column = chunk * CHUNK + lax.broadcasted_iota(jnp.int32, scores.shape, 1)
        scores = jnp.where(column <= row, scores, BIG)
        peak = jnp.max(scores, axis=1, keepdims=True)
        weights = jnp.exp2((scores - peak) * factor)
        top[half] = jnp.broadcast_to(peak, top.shape[1:])
        norm[half] = jnp.broadcast_to(jnp.sum(weights, axis=1, keepdims=True), norm.shape[1:])
        acc[half] = times_values(weights, chunk)

    def step(i, carry):
        there = NCHUNK - 1 - ci
        half = jnp.where(i < there, 1, 0)
        chunk = jnp.where(i < there, i, i - there)
        scores = scores_of(half, chunk)
        before = top[half]
        peak = jnp.maximum(before, jnp.max(scores, axis=1, keepdims=True))
        wide = jnp.concatenate([peak] * (CHUNK // 128), axis=1)
        weights = jnp.exp2((scores - wide) * factor)
        fade = jnp.exp2((before - peak) * factor)
        top[half] = peak
        norm[half] = norm[half] * fade + jnp.sum(weights, axis=1, keepdims=True)
        acc[half] = acc[half] * fade + times_values(weights, chunk)
        return carry

    far = NCHUNK - 1 - ci
    diagonal(1, far, far * CHUNK + c * BLK + HALF)
    diagonal(0, ci, ci * CHUNK + c * BLK)
    waiting = merged(wa, wb)
    cuts = [0, 8, 16, 24, 31]
    for lo, hi in zip(cuts[:-1], cuts[1:]):
        lax.fori_loop(lo, hi, step, 0)
        take = 6
        for _, g, dx, dz, sends in waiting[:take]:
            g.run(dx, dz, sends)
        waiting = waiting[take:]

    mine = heads_at(0)
    result = (acc[1] / norm[1]).astype(jnp.bfloat16)
    for head in range(GROUP):
        back[:, head * HEAD_DIM : (head + 1) * HEAD_DIM] = result[head * HALF : (head + 1) * HALF]
    low, high = pl.ds(0, HALF), pl.ds(HALF, HALF)
    act_copies = []

    def act_send_to(slot, source, dest, target):
        copy = pltpu.make_async_remote_copy(
            src_ref=source, dst_ref=dest, send_sem=act_send.at[slot], recv_sem=act_recv.at[slot],
            device_id=target, device_id_type=MESH,
        )
        copy.start()
        act_copies.append(copy)
        return copy

    home = act_send_to(0, back, backin, flip)
    result = (acc[0] / norm[0]).astype(jnp.bfloat16)
    for head in range(GROUP):
        acts[mine, 0:HALF, head * HEAD_DIM : (head + 1) * HEAD_DIM] = result[head * HALF : (head + 1) * HALF]
    low_up = act_send_to(1, acts.at[mine, low], acts.at[mine, low], along_y(1))
    low_down = act_send_to(2, acts.at[mine, low], acts.at[mine, low], along_y(-1))
    home.wait_recv()
    acts[mine, HALF:BLK, :] = backin[...]
    high_up = act_send_to(3, backin, acts.at[mine, high], along_y(1))
    high_down = act_send_to(4, backin, acts.at[mine, high], along_y(-1))

    for _, g, dx, dz, sends in waiting[: 12]:
        g.run(dx, dz, sends)
    waiting = waiting[12:]
    below, above = heads_at(-1), heads_at(1)
    low_up.wait_recv()
    low_on = act_send_to(5, acts.at[below, low], acts.at[below, low], along_y(1))
    low_down.wait_recv()
    high_up.wait_recv()
    high_down.wait_recv()
    high_on = act_send_to(6, acts.at[above, high], acts.at[above, high], along_y(-1))
    for _, g, dx, dz, sends in waiting:
        g.run(dx, dz, sends)
    low_on.wait_recv()
    high_on.wait_recv()
    wa.finish_sides()
    wb.finish_sides()

    def project(zi, carry):
        total = jnp.zeros((BLK, 256), jnp.float32)
        for kk in range(NX):
            i = kk * NZ + zi
            both = jnp.concatenate([wall[i, 0], wall[i, 1]], axis=1)
            total = total + jnp.dot(acts[kk], both, preferred_element_type=jnp.float32)
        out_ref[:, pl.ds(pl.multiple_of(zi * 256, 256), 256)] = total.astype(jnp.bfloat16)
        return carry

    lax.fori_loop(0, NZ, project, 0)
    for g in (vg, kg, wa, wb):
        g.finish_sends()
    for copy in act_copies:
        copy.wait_send()


def main_call(q, pen, k, v, bounds, w):
    rows = GROUP * HALF
    return pl.pallas_call(
        main_kernel,
        out_shape=jax.ShapeDtypeStruct((BLK, 2048), jnp.bfloat16),
        in_specs=[pl.BlockSpec(memory_space=pltpu.VMEM)] * 6,
        out_specs=pl.BlockSpec(memory_space=pltpu.VMEM),
        scratch_shapes=[
            pltpu.VMEM((NCHUNK, 2, BLK, HEAD_DIM), jnp.bfloat16),
            pltpu.VMEM((NCHUNK, 2, BLK, HEAD_DIM), jnp.bfloat16),
            pltpu.VMEM((NCHUNK, CHUNK, 128), jnp.bfloat16),
            pltpu.VMEM((NCHUNK, 2, WROWS, 128), jnp.bfloat16),
            pltpu.VMEM((2, rows, 2 * HEAD_DIM), jnp.bfloat16),
            pltpu.VMEM((2, rows, 128), jnp.float32),
            pltpu.VMEM((2, rows, 128), jnp.float32),
            pltpu.VMEM((2, rows, HEAD_DIM), jnp.float32),
            pltpu.VMEM((4, BLK, GROUP * HEAD_DIM), jnp.bfloat16),
            pltpu.VMEM((HALF, GROUP * HEAD_DIM), jnp.bfloat16),
            pltpu.VMEM((HALF, GROUP * HEAD_DIM), jnp.bfloat16),
            pltpu.SemaphoreType.DMA((4, NCHUNK)),
            pltpu.SemaphoreType.DMA((4, NCHUNK)),
            pltpu.SemaphoreType.DMA((4, 64)),
            pltpu.SemaphoreType.DMA((7,)),
            pltpu.SemaphoreType.DMA((7,)),
        ],
        compiler_params=pltpu.CompilerParams(
            collective_id=2, has_side_effects=True, vmem_limit_bytes=60 * 1024 * 1024
        ),
        name="attend_project",
    )(q, pen, k, v, bounds, w)


def rotate_heads(inputs, positions):
    row_count = inputs.shape[0]
    head_count = inputs.shape[1] // HEAD_DIM
    half_dim = HEAD_DIM // 2
    widened = inputs.astype(jnp.float32).reshape(row_count, head_count, HEAD_DIM)
    exponent = jnp.arange(half_dim, dtype=jnp.float32) * (2.0 / HEAD_DIM)
    inverse = jnp.power(jnp.float32(ROPE_BASE), -exponent)
    angles = positions.astype(jnp.float32)[:, None] * inverse[None, :]
    cosine_table = jnp.cos(angles)[:, None, :]
    sine_table = jnp.sin(angles)[:, None, :]
    first_half = widened[:, :, :half_dim]
    second_half = widened[:, :, half_dim:]
    turned = jnp.concatenate(
        [
            first_half * cosine_table - second_half * sine_table,
            second_half * cosine_table + first_half * sine_table,
        ],
        axis=2,
    )
    return turned.reshape(row_count, head_count * HEAD_DIM).astype(jnp.bfloat16)


def local(queries, keys, values, segment_ids, out_weight):
    both = ("seq", "tp")
    swap = route(swap_to)
    labels = jnp.arange(128, dtype=jnp.int32)
    counts = jnp.sum((segment_ids[:, None] == labels[None, :]).astype(jnp.int32), axis=0)
    keys = lax.ppermute(keys, both, swap)
    values = lax.ppermute(values, both, swap)
    lower = lax.ppermute(queries[:HALF], both, swap)
    upper = lax.ppermute(queries[HALF:], both, route(flip_swap_to))
    weight = lax.ppermute(out_weight, both, route(weight_to))
    totals = counts_total(jnp.broadcast_to(counts[None, :], (8, 128)))[0]
    ends = jnp.cumsum(totals[:SEGMENTS])
    starts = ends - totals[:SEGMENTS]

    x, z, _, _, c = coords(lax.axis_index("seq"), lax.axis_index("tp"))
    block = (x * NZ + z) * 2 + c
    mirror = ((NX - 1 - x) * NZ + NZ - 1 - z) * 2 + c
    key_rows = block * BLK + jnp.arange(BLK, dtype=jnp.int32)
    upper_rows = mirror * BLK + HALF + jnp.arange(HALF, dtype=jnp.int32)

    def place(rows):
        past = ends[None, :] <= rows[:, None]
        segment = jnp.sum(past.astype(jnp.int32), axis=1)
        return segment, rows - jnp.max(jnp.where(past, ends[None, :], 0), axis=1)

    key_segment, key_position = place(key_rows)
    upper_segment, upper_position = place(upper_rows)
    query_rot = jnp.concatenate(
        [rotate_heads(lower, key_position[:HALF]), rotate_heads(upper, upper_position)], axis=0
    )
    key_rot = rotate_heads(keys, key_position)
    segment = jnp.concatenate([key_segment[:HALF], upper_segment])
    hidden = (labels[None, :] != segment[:, None]) & (labels[None, :] < SEGMENTS)
    penalty = jnp.where(hidden, BIG, 0.0).astype(jnp.bfloat16)
    far = jnp.full((128 - SEGMENTS,), 1 << 30, jnp.int32)
    bounds = jnp.stack([jnp.concatenate([starts, far]), jnp.concatenate([ends, far])])
    bounds = jnp.concatenate([bounds, jnp.zeros((6, 128), jnp.int32)], axis=0)
    tile = main_call(query_rot, penalty, key_rot, values, bounds, weight)
    return lax.ppermute(tile, both, swap)


def solution(mesh):
    return jax.shard_map(
        local,
        mesh=mesh,
        in_specs=(P("seq", "tp"), P("seq", "tp"), P("seq", "tp"), P("seq"), P("tp", "seq")),
        out_specs=P("seq", "tp"),
        check_vma=False,
    )
```

```python
import functools
import math

import jax
import jax.numpy as jnp
from jax import lax
from jax.experimental import pallas as pl
from jax.experimental.pallas import tpu as pltpu
from jax.sharding import PartitionSpec as P

HEAD_DIM = 128
SEGMENTS = 16
NX, NZ = 4, 8
BLK = 192
HALF = 96
GROUP = 8
CHUNK = 384
NCHUNK = 32
WROWS = 1024
WSPLIT = 448
ROPE_BASE = 500000.0
BIG = -1e30
MESH = pl.DeviceIdType.MESH


def coords(j, k):
    return j // 16, (j // 2) % 8, j % 2, k // 2, k % 2


def seq_tp(x, z, h, yl, c):
    return x * 16 + z * 2 + h, yl * 2 + c


def here():
    j = lax.axis_index("seq")
    k = lax.axis_index("tp")
    return coords(j, k)


def ident(x, z, h, yl, c):
    return {"seq": x * 16 + z * 2 + h, "tp": yl * 2 + c}


def mod(value, n):
    return lax.rem(value + 2 * n, n)


ORDER = (0, -1, 1, -2, 2, -3, 3, -4)


class Gather:
    def __init__(self, slot, first_axis, place, own, ring_sem, side_sem, send_sem):
        self.slot, self.first_axis, self.place, self.own = slot, first_axis, place, own
        self.ring_sem, self.side_sem, self.send_sem = ring_sem, side_sem, send_sem
        self.sent = []
        self.done = set()
        self.x, self.z, self.h, self.yl, self.c = here()

    def chunk(self, dx, dz):
        return mod(self.x + dx, NX) * NZ + mod(self.z + dz, NZ)

    def send(self, dx, dz, axis, step):
        ci = self.chunk(dx, dz)
        there = self.place(ci, self.c)
        source = self.own if (dx, dz) == (0, 0) else there
        recv = self.side_sem if axis == "side" else self.ring_sem
        if axis == "side":
            target = ident(self.x, self.z, self.h, self.yl, 1 - self.c)
        elif axis == "x":
            target = ident(mod(self.x + step, NX), self.z, self.h, self.yl, self.c)
        else:
            target = ident(self.x, mod(self.z + step, NZ), self.h, self.yl, self.c)
        copy = pltpu.make_async_remote_copy(
            src_ref=source, dst_ref=there, send_sem=self.send_sem.at[self.slot, len(self.sent)],
            recv_sem=recv.at[self.slot, ci], device_id=target, device_id_type=MESH,
        )
        copy.start()
        self.sent.append(copy)

    def arrived(self, dx, dz, side=False):
        ci = self.chunk(dx, dz)
        sem = self.side_sem if side else self.ring_sem
        ref = self.place(ci, 1 - self.c if side else self.c)
        pltpu.make_async_remote_copy(
            src_ref=ref, dst_ref=ref, send_sem=self.send_sem.at[self.slot, 0], recv_sem=sem.at[self.slot, ci],
            device_id=ident(self.x, self.z, self.h, self.yl, 1 - self.c), device_id_type=MESH,
        ).wait_recv()

    def begin(self, *axes):
        for axis in axes:
            if axis == "side":
                self.send(0, 0, "side", 0)
            else:
                self.send(0, 0, axis, 1)
                self.send(0, 0, axis, -1)

    def onward(self, dx, dz):
        s = abs(dz)
        if self.first_axis == "z":
            if dx == 0:
                keep = (dz < 0 and s <= 3) or (dz > 0 and s <= 2)
                return ([("z", 1 if dz < 0 else -1)] if keep else []), [("x", 1), ("x", -1)]
            first = dz % 8 < 4
            return ([("x", 1)] if dx == -1 and first else [("x", -1)] if dx == 1 and not first else []), []
        if dz == 0:
            return ([("x", 1)] if dx == -1 else []), [("z", 1), ("z", -1)]
        first = dx in (0, 1)
        if dz < 0:
            return ([("z", 1)] if s <= 2 or (s == 3 and first) else []), []
        return ([("z", -1)] if s <= 2 or (s == 3 and not first) else []), []

    def run(self, dx, dz, cross=True):
        if (dx, dz) in self.done:
            return
        self.done.add((dx, dz))
        along, over = self.onward(dx, dz)
        if self.first_axis == "x" and dz == -4 and dx not in (0, 1):
            along = []
        self.arrived(dx, dz)
        for axis, step in along + (over if cross else []):
            self.send(dx, dz, axis, step)
        self.send(dx, dz, "side", 0)

    def finish_sends(self):
        for copy in self.sent:
            copy.wait_send()


def main_kernel(
    q_ref, k_ref, v_ref, seg_ref, freq_ref, w_ref, out_ref,
    kin, vin, krot, win, qin, kall, vall, tags, wall, qa, top, norm, acc, acts, back, backin, obuf, cown, cpart, cgot,
    ring_sem, side_sem, send_sem, act_send, act_recv, in_send, in_recv, cnt_send, cnt_recv, out_send, out_recv,
):
    x, z, h, yl, c = here()
    y = 2 * h + yl
    ci = x * NZ + z
    far = NCHUNK - 1 - ci
    side = ident(x, z, h, yl, 1 - c)
    flip = ident(NX - 1 - x, NZ - 1 - z, h, yl, c)
    swap = ident(x, z, c, yl, h)
    flip_swap = ident(NX - 1 - x, NZ - 1 - z, c, yl, h)
    w_dest = ident(2 * yl + h, z, lax.rem(x, 2), x // 2, c)
    keeps = h == c
    keeps_w = x == 2 * yl + h

    def along_y(step):
        there = mod(y + step, 4)
        return ident(x, z, there // 2, lax.rem(there, 2), c)

    def heads_at(step):
        there = mod(y + step, 4)
        return 2 * lax.rem(there, 2) + there // 2

    by_z = [ident(x, mod(z + d, NZ), h, yl, c) for d in range(1, NZ)]
    by_x = [ident(mod(x + d, NX), z, h, yl, c) for d in range(1, NX)]
    by_h = [ident(x, z, 1 - h, yl, c)]
    barrier = pltpu.get_barrier_semaphore()
    always = by_z + by_x + by_h + [along_y(1), along_y(-1), side, flip, flip_swap, swap, w_dest]
    for peer in always:
        pl.semaphore_signal(barrier, inc=1, device_id=peer, device_id_type=MESH)
    labels = lax.broadcasted_iota(jnp.int32, (BLK, 128), 1)
    own_counts = jnp.sum(jnp.where(seg_ref[...] == labels, 1.0, 0.0), axis=0, keepdims=True)
    cown[...] = jnp.broadcast_to(own_counts, (8, 128)).astype(jnp.int32)
    pl.semaphore_wait(barrier, len(always))

    def remote(slot, source, dest, target, send, recv):
        return pltpu.make_async_remote_copy(
            src_ref=source, dst_ref=dest, send_sem=send.at[slot], recv_sem=recv.at[slot],
            device_id=target, device_id_type=MESH,
        )

    def count_phase(at, source, peers, between):
        copies = [remote(at + i, source, cgot.at[at + i], p, cnt_send, cnt_recv) for i, p in enumerate(peers)]
        for copy in copies:
            copy.start()
        between()
        total = source[...]
        for i, copy in enumerate(copies):
            copy.wait()
            total = total + cgot[at + i]
        return total

    low, high = pl.ds(0, HALF), pl.ds(HALF, HALF)
    moved = {
        "v": (keeps, remote(0, v_ref, vin, swap, in_send, in_recv)),
        "k": (keeps, remote(1, k_ref, kin, swap, in_send, in_recv)),
        "q": (keeps, remote(2, q_ref.at[low], qin.at[low], swap, in_send, in_recv)),
        "w": (keeps_w, remote(3, w_ref, win, w_dest, in_send, in_recv)),
    }
    own_copy = {
        "v": lambda: vin.__setitem__(..., v_ref[...]),
        "k": lambda: kin.__setitem__(..., k_ref[...]),
        "q": lambda: qin.__setitem__((low, slice(None)), q_ref[low, :]),
        "w": lambda: win.__setitem__(..., w_ref[...]),
    }
    upper = remote(4, q_ref.at[high], qin.at[high], flip_swap, in_send, in_recv)

    def start_move(name):
        own, copy = moved[name]
        pl.when(own)(own_copy[name])
        pl.when(jnp.logical_not(own))(copy.start)

    def end_move(name):
        own, copy = moved[name]
        pl.when(jnp.logical_not(own))(copy.wait_recv)

    sems = (ring_sem, side_sem, send_sem)
    vg = Gather(0, "z", lambda i, t: vall.at[i, t], vin, *sems)
    kg = Gather(1, "z", lambda i, t: kall.at[i, t], krot, *sems)
    wa = Gather(2, "z", lambda i, t: wall.at[i, t, pl.ds(0, WSPLIT)], win.at[pl.ds(0, WSPLIT)], *sems)
    wb = Gather(3, "x", lambda i, t: wall.at[i, t, pl.ds(WSPLIT, WROWS - WSPLIT)],
                win.at[pl.ds(WSPLIT, WROWS - WSPLIT)], *sems)

    def first_moves():
        start_move("v")
        start_move("k")

    def second_moves():
        end_move("v")
        vg.begin("z", "x", "side")
        vall[ci, c] = vin[...]

    def third_moves():
        start_move("q")
        upper.start()
        start_move("w")

    cpart[0] = count_phase(0, cown, by_z, first_moves)
    cpart[1] = count_phase(7, cpart.at[0], by_x, second_moves)
    totals = count_phase(10, cpart.at[1], by_h, third_moves)[0:1].astype(jnp.float32)
    lane = lax.broadcasted_iota(jnp.int32, (1, 128), 1)
    ends = totals
    for shift in (1, 2, 4, 8, 16, 32, 64):
        ends = ends + jnp.where(lane >= shift, pltpu.roll(ends, shift, 1), 0.0)
    starts = ends - totals

    def rows_from(first, count):
        return (first + lax.broadcasted_iota(jnp.int32, (count, 128), 0)).astype(jnp.float32)

    def turns(first, count):
        rows = rows_from(first, count)
        start = jnp.max(jnp.where(ends <= rows, ends, 0.0), axis=1, keepdims=True)
        angles = (rows - start) * freq_ref[0:1, :]
        sine = jnp.sin(angles)
        lanes = lax.broadcasted_iota(jnp.int32, (count, 128), 1)
        return jnp.cos(angles), jnp.where(lanes < HEAD_DIM // 2, -sine, sine)

    def rotated(block, cosine, sine):
        wide = block.astype(jnp.float32)
        return (wide * cosine + pltpu.roll(wide, HEAD_DIM // 2, 1) * sine).astype(jnp.bfloat16)

    first_key = ci * CHUNK + c * BLK
    key_cos, key_sin = turns(first_key, BLK)
    end_move("k")
    krot[...] = rotated(kin[...], key_cos, key_sin)
    kg.begin("z", "x", "side")
    kall[ci, c] = krot[...]
    top[...] = jnp.full(top.shape, BIG, jnp.float32)
    norm[...] = jnp.zeros_like(norm)
    acc[...] = jnp.zeros_like(acc)

    def inside(rows):
        return (rows >= starts) & (rows < ends)

    def tag(i, carry):
        tags[i] = jnp.where(inside(rows_from(i * CHUNK, CHUNK)), 1.0, 0.0).astype(jnp.bfloat16)
        return carry

    for dz in ORDER[1:3]:
        vg.run(0, dz)
    lax.fori_loop(0, NCHUNK, tag, 0)
    end_move("w")
    for dz in ORDER[1:3]:
        kg.run(0, dz)
    wb.begin("x")
    for dz in ORDER[3:5]:
        vg.run(0, dz)
    up_cos, up_sin = turns(far * CHUNK + c * BLK + HALF, HALF)
    upper.wait_recv()
    end_move("q")
    for half, (cosine, sine) in enumerate(((key_cos[:HALF], key_sin[:HALF]), (up_cos, up_sin))):
        rows = pl.ds(half * HALF, HALF)
        first_row = ci * CHUNK + c * BLK if half == 0 else far * CHUNK + c * BLK + HALF
        lanes = lax.broadcasted_iota(jnp.int32, (HALF, 128), 1)
        hidden = jnp.logical_not(inside(rows_from(first_row, HALF))) & (lanes < SEGMENTS)
        penalty = jnp.where(hidden, BIG, 0.0).astype(jnp.bfloat16)
        for head in range(GROUP):
            at = pl.ds(head * HALF, HALF)
            qa[half, at, 0:HEAD_DIM] = rotated(qin[rows, head * HEAD_DIM : (head + 1) * HEAD_DIM], cosine, sine)
            qa[half, at, HEAD_DIM : 2 * HEAD_DIM] = penalty
    for dz in ORDER[3:5]:
        kg.run(0, dz)
    for dz in ORDER[5:8]:
        vg.run(0, dz)
    for dz in ORDER[5:8]:
        kg.run(0, dz)
    wall[ci, c] = win[...]
    wa.begin("z", "side")
    wb.begin("z", "side")

    factor = math.log2(math.e) / math.sqrt(HEAD_DIM)

    def attend(half, chunk, mask_from=None):
        keys = jnp.concatenate([kall[chunk].reshape(CHUNK, HEAD_DIM), tags[chunk]], axis=1)
        vals = vall[chunk].reshape(CHUNK, HEAD_DIM)
        size = GROUP * HALF // 2
        tiles = [pl.ds(r, size) for r in range(0, GROUP * HALF, size)]
        olds = [(top[half, r], norm[half, r], acc[half, r]) for r in tiles]

        def scored(r):
            found = lax.dot_general(
                qa[half, r], keys, (((1,), (1,)), ((), ())), preferred_element_type=jnp.float32
            )
            if mask_from is not None:
                row = lax.rem(lax.broadcasted_iota(jnp.int32, found.shape, 0), HALF) + mask_from
                column = chunk * CHUNK + lax.broadcasted_iota(jnp.int32, found.shape, 1)
                found = jnp.where(column <= row, found, BIG)
            return found

        ahead = scored(tiles[0])
        news = []
        for n in range(len(tiles)):
            scores = ahead
            if n + 1 < len(tiles):
                ahead = scored(tiles[n + 1])
            before, total, mix = olds[n]
            peak = jnp.maximum(before, jnp.max(scores, axis=1, keepdims=True))
            fade = jnp.exp2((before - peak) * factor)
            parts = [jnp.exp2((scores[:, i : i + 128] - peak) * factor) for i in range(0, CHUNK, 128)]
            weights = jnp.concatenate([p.astype(jnp.bfloat16) for p in parts], axis=1)
            added = jnp.dot(weights, vals, preferred_element_type=jnp.float32)
            news.append((peak, total * fade + sum(parts[1:], parts[0]), mix * fade + added))
        for r, (a, b, d) in zip(tiles, news):
            top[half, r] = a
            norm[half, r] = b
            acc[half, r] = d

    def row_steps(dx, pieces):
        base = mod(x + dx, NX) * NZ
        n1 = jnp.clip(far - base, 0, NZ)
        total = n1 + jnp.clip(ci - base, 0, NZ)

        def step(i, carry):
            upper_half = i < n1
            attend(jnp.where(upper_half, 1, 0), base + jnp.where(upper_half, i, i - n1))
            return carry

        for p in range(pieces):
            yield lambda p=p: lax.fori_loop(total * p // pieces, total * (p + 1) // pieces, step, 0)

    def row_ready(dx):
        for dz in ORDER:
            for g in (vg, kg):
                g.arrived(dx, dz, side=True)

    def both(dx, dz):
        vg.run(dx, dz)
        kg.run(dx, dz)

    row_ready(0)
    attend(0, ci, ci * CHUNK + c * BLK)
    for p, go in enumerate(row_steps(0, 4)):
        go()
        for dz in ORDER[p : p + 1]:
            both(-1, dz)
            both(1, dz)
        if p == 1:
            for dx in (-1, 1, 2):
                wb.run(dx, 0)
        if p >= 2:
            for dz in ORDER[1:3] if p == 2 else ORDER[3:5]:
                wa.run(0, dz, cross=False)
    for p in range(4, 8):
        both(-1, ORDER[p])
        both(1, ORDER[p])
        both(2, ORDER[p - 4])
    for dz in ORDER[5:8]:
        wa.run(0, dz, cross=False)
    wa.begin("x")
    for dz in ORDER[1:8]:
        wa.send(0, dz, "x", 1)
        wa.send(0, dz, "x", -1)
    due = []
    for s in range(1, 5):
        for dx in (0, -1, 1, 2):
            if s < 4:
                due += [(wb, dx, -s), (wb, dx, s)]
            else:
                due.append((wb, dx, -4 if dx in (0, 1) else 4))

    def take(n):
        for g, dx, dz in due[:n]:
            g.run(dx, dz)
        del due[:n]

    row_ready(-1)
    for p, go in enumerate(row_steps(-1, 3)):
        go()
        take(2)
        if p < 2:
            both(2, ORDER[4 + p])
    row_ready(1)
    attend(1, far, far * CHUNK + c * BLK + HALF)
    for p, go in enumerate(row_steps(1, 3)):
        go()
        take(2)
        if p < 2:
            both(2, ORDER[6 + p])
    row_ready(2)
    for p, go in enumerate(row_steps(2, 3)):
        go()
        take(1)

    mine = heads_at(0)

    def finished(half):
        total = jnp.sum(norm[half], axis=1, keepdims=True)
        return (acc[half] / total).astype(jnp.bfloat16)

    act_copies = []

    def act_start(slot, source, dest, target):
        copy = remote(slot, source, dest, target, act_send, act_recv)
        copy.start()
        act_copies.append(copy)
        return copy

    result = finished(1)
    for head in range(GROUP):
        back[:, head * HEAD_DIM : (head + 1) * HEAD_DIM] = result[head * HALF : (head + 1) * HALF]
    home = act_start(0, back, backin, flip)
    result = finished(0)
    for head in range(GROUP):
        acts[mine, 0:HALF, head * HEAD_DIM : (head + 1) * HEAD_DIM] = result[head * HALF : (head + 1) * HALF]
    low_up = act_start(1, acts.at[mine, low], acts.at[mine, low], along_y(1))
    low_down = act_start(2, acts.at[mine, low], acts.at[mine, low], along_y(-1))
    take(3)
    for dz in ORDER[:2]:
        wa.run(-1, dz)
        wa.run(1, dz)
    home.wait_recv()
    acts[mine, HALF:BLK, :] = backin[...]
    high_up = act_start(3, backin, acts.at[mine, high], along_y(1))
    high_down = act_start(4, backin, acts.at[mine, high], along_y(-1))
    take(2)
    for dz in ORDER[2:4]:
        wa.run(-1, dz)
        wa.run(1, dz)
    below, above = heads_at(-1), heads_at(1)
    low_up.wait_recv()
    low_on = act_start(5, acts.at[below, low], acts.at[below, low], along_y(1))
    take(3)
    high_down.wait_recv()
    high_on = act_start(6, acts.at[above, high], acts.at[above, high], along_y(-1))
    low_down.wait_recv()
    high_up.wait_recv()
    take(3)
    for dz in ORDER[:2]:
        wa.run(2, dz)
    for dz in ORDER[4:6]:
        wa.run(-1, dz)
        wa.run(1, dz)
    low_on.wait_recv()
    high_on.wait_recv()

    given = []
    for dz in ORDER:
        zi = mod(z + dz, NZ)
        for dx in (-1, 1, 2):
            wa.run(dx, dz)
        far_dz = dz
        for dx in (0, -1, 1, 2):
            if abs(dz) == 4:
                far_dz = -4 if dx in (0, 1) else 4
            if (dx, dz) != (0, 0):
                wb.run(dx, far_dz)
        for dx in (0, -1, 1, 2):
            wa.arrived(dx, dz, side=True)
            wb.arrived(dx, dz, side=True)
        total = jnp.zeros((BLK, 256), jnp.float32)
        for kk in range(NX):
            pair = [wall[(2 * (kk // 2) + t) * NZ + zi, kk % 2] for t in range(2)]
            total = total + jnp.dot(acts[kk], jnp.concatenate(pair, axis=1), preferred_element_type=jnp.float32)
        block = total.astype(jnp.bfloat16)
        copy = remote(zi, obuf.at[zi], out_ref.at[zi], swap, out_send, out_recv)
        given.append(copy)

        @pl.when(keeps)
        def _(zi=zi, block=block):
            out_ref[zi] = block

        @pl.when(jnp.logical_not(keeps))
        def _(zi=zi, block=block, copy=copy):
            obuf[zi] = block
            copy.start()

    for g in (vg, kg, wa, wb):
        g.finish_sends()
    for copy in act_copies:
        copy.wait_send()
    upper.wait_send()
    for own, copy in moved.values():
        pl.when(jnp.logical_not(own))(copy.wait_send)

    @pl.when(jnp.logical_not(keeps))
    def _():
        for copy in given:
            copy.wait()


def main_call(q, k, v, seg, freq, w):
    rows = GROUP * HALF
    return pl.pallas_call(
        main_kernel,
        out_shape=jax.ShapeDtypeStruct((NZ, BLK, 256), jnp.bfloat16),
        in_specs=[pl.BlockSpec(memory_space=pltpu.VMEM)] * 6,
        out_specs=pl.BlockSpec(memory_space=pltpu.VMEM),
        scratch_shapes=[
            pltpu.VMEM((BLK, HEAD_DIM), jnp.bfloat16),
            pltpu.VMEM((BLK, HEAD_DIM), jnp.bfloat16),
            pltpu.VMEM((BLK, HEAD_DIM), jnp.bfloat16),
            pltpu.VMEM((WROWS, 128), jnp.bfloat16),
            pltpu.VMEM((BLK, GROUP * HEAD_DIM), jnp.bfloat16),
            pltpu.VMEM((NCHUNK, 2, BLK, HEAD_DIM), jnp.bfloat16),
            pltpu.VMEM((NCHUNK, 2, BLK, HEAD_DIM), jnp.bfloat16),
            pltpu.VMEM((NCHUNK, CHUNK, 128), jnp.bfloat16),
            pltpu.VMEM((NCHUNK, 2, WROWS, 128), jnp.bfloat16),
            pltpu.VMEM((2, rows, 2 * HEAD_DIM), jnp.bfloat16),
            pltpu.VMEM((2, rows, 128), jnp.float32),
            pltpu.VMEM((2, rows, 128), jnp.float32),
            pltpu.VMEM((2, rows, HEAD_DIM), jnp.float32),
            pltpu.VMEM((4, BLK, GROUP * HEAD_DIM), jnp.bfloat16),
            pltpu.VMEM((HALF, GROUP * HEAD_DIM), jnp.bfloat16),
            pltpu.VMEM((HALF, GROUP * HEAD_DIM), jnp.bfloat16),
            pltpu.VMEM((NZ, BLK, 256), jnp.bfloat16),
            pltpu.VMEM((8, 128), jnp.int32),
            pltpu.VMEM((2, 8, 128), jnp.int32),
            pltpu.VMEM((11, 8, 128), jnp.int32),
            pltpu.SemaphoreType.DMA((4, NCHUNK)),
            pltpu.SemaphoreType.DMA((4, NCHUNK)),
            pltpu.SemaphoreType.DMA((4, 64)),
            pltpu.SemaphoreType.DMA((7,)),
            pltpu.SemaphoreType.DMA((7,)),
            pltpu.SemaphoreType.DMA((5,)),
            pltpu.SemaphoreType.DMA((5,)),
            pltpu.SemaphoreType.DMA((11,)),
            pltpu.SemaphoreType.DMA((11,)),
            pltpu.SemaphoreType.DMA((NZ,)),
            pltpu.SemaphoreType.DMA((NZ,)),
        ],
        compiler_params=pltpu.CompilerParams(
            collective_id=2, has_side_effects=True, vmem_limit_bytes=60 * 1024 * 1024
        ),
        name="attend_project",
    )(q, k, v, seg, freq, w)


def local(queries, keys, values, segment_ids, out_weight):
    half_dim = HEAD_DIM // 2
    exponent = jnp.arange(half_dim, dtype=jnp.float32) * (2.0 / HEAD_DIM)
    inverse = jnp.power(jnp.float32(ROPE_BASE), -exponent)
    freq = jnp.broadcast_to(jnp.concatenate([inverse, inverse])[None, :], (8, HEAD_DIM))
    segments = jnp.broadcast_to(segment_ids[:, None], (BLK, 128))
    tile = main_call(queries, keys, values, segments, freq, out_weight)
    return jnp.transpose(tile, (1, 0, 2)).reshape(BLK, NZ * 256)


def solution(mesh):
    return jax.shard_map(
        local,
        mesh=mesh,
        in_specs=(P("seq", "tp"), P("seq", "tp"), P("seq", "tp"), P("seq"), P("tp", "seq")),
        out_specs=P("seq", "tp"),
        check_vma=False,
    )
```

```python
import functools
import math

import jax
import jax.numpy as jnp
from jax import lax
from jax.experimental import pallas as pl
from jax.experimental.pallas import tpu as pltpu
from jax.sharding import PartitionSpec as P

HEAD_DIM = 128
SEGMENTS = 16
NX, NZ = 4, 8
BLK = 192
HALF = 96
GROUP = 8
CHUNK = 384
NCHUNK = 32
WROWS = 1024
WSPLIT = 560
ROPE_BASE = 500000.0
BIG = -1e30
MESH = pl.DeviceIdType.MESH


def coords(j, k):
    return j // 16, (j // 2) % 8, j % 2, k // 2, k % 2


def seq_tp(x, z, h, yl, c):
    return x * 16 + z * 2 + h, yl * 2 + c


def here():
    j = lax.axis_index("seq")
    k = lax.axis_index("tp")
    return coords(j, k)


def ident(x, z, h, yl, c):
    return {"seq": x * 16 + z * 2 + h, "tp": yl * 2 + c}


def mod(value, n):
    return lax.rem(value + 2 * n, n)


ORDER = (0, -1, 1, -2, 2, -3, 3, -4)
LINK_KB_PER_US = 40.0
HOP_US = 2.2


class Plan:
    def __init__(self):
        self.put_off = []
        self.now, self.free, self.events, self.done, self.held = 0.0, {}, [], set(), False

    def sent(self, link, size, key, arrive):
        start = max(self.now, self.free.get(link, 0.0))
        self.free[link] = start + size / LINK_KB_PER_US
        self.events.append((self.free[link] + HOP_US, len(self.events), key, arrive))

    def take(self, event):
        self.events = [e if e is not event else (1e9, e[1], None, None) for e in self.events]
        self.now = max(self.now, event[0]) + 0.03
        self.done.add(event[2])
        event[3]()

    def late(self, key):
        return (key[0] == 2 and key[1] != 0) or (key[0] == 3 and key[2] != 0)

    def release(self):
        self.held = False
        for again in self.put_off:
            again()
        self.poll()

    def first(self):
        return min((e for e in self.events if e[2] and not (self.held and self.late(e[2]))), default=(1e9, 0, None, None))

    def poll(self, spent=0.0):
        self.now += spent
        while self.first()[0] <= self.now - 0.5:
            self.take(self.first())

    def until(self, keys):
        while not set(keys) <= self.done:
            self.take(self.first())


class Gather:
    def __init__(self, plan, slot, first_axis, size, place, own, ring_sem, side_sem, send_sem):
        self.plan, self.slot, self.first_axis, self.size, self.place, self.own = plan, slot, first_axis, size, place, own
        self.ring_sem, self.side_sem, self.send_sem = ring_sem, side_sem, send_sem
        self.sent = []
        self.x, self.z, self.h, self.yl, self.c = here()

    def key(self, dx, dz):
        return self.slot, dx % NX, dz % NZ

    def keys(self):
        return [self.key(dx, dz) for dx in range(NX) for dz in range(NZ) if dx or dz]

    def chunk(self, dx, dz):
        return mod(self.x + dx, NX) * NZ + mod(self.z + dz, NZ)

    def send(self, dx, dz, axis, step):
        if self.plan.held and self.slot > 1 and axis not in ("side", self.first_axis):
            self.plan.put_off.append(lambda: self.send(dx, dz, axis, step))
            return
        ci = self.chunk(dx, dz)
        there = self.place(ci, self.c)
        source = self.own if (dx, dz) == (0, 0) else there
        recv = self.side_sem if axis == "side" else self.ring_sem
        if axis == "side":
            target = ident(self.x, self.z, self.h, self.yl, 1 - self.c)
        elif axis == "x":
            target = ident(mod(self.x + step, NX), self.z, self.h, self.yl, self.c)
        else:
            target = ident(self.x, mod(self.z + step, NZ), self.h, self.yl, self.c)
        copy = pltpu.make_async_remote_copy(
            src_ref=source, dst_ref=there, send_sem=self.send_sem.at[self.slot, len(self.sent)],
            recv_sem=recv.at[self.slot, ci], device_id=target, device_id_type=MESH,
        )
        copy.start()
        self.sent.append(copy)
        if axis != "side":
            seen = (dx - step, dz) if axis == "x" else (dx, dz - step)
            seen = (2 if seen[0] == -2 else seen[0], seen[1])
            self.plan.sent((axis, 1 if step > 0 else -1), self.size * abs(step), self.key(*seen), lambda: self.run(*seen))

    def arrived(self, dx, dz, side=False):
        ci = self.chunk(dx, dz)
        sem = self.side_sem if side else self.ring_sem
        ref = self.place(ci, 1 - self.c if side else self.c)
        pltpu.make_async_remote_copy(
            src_ref=ref, dst_ref=ref, send_sem=self.send_sem.at[self.slot, 0], recv_sem=sem.at[self.slot, ci],
            device_id=ident(self.x, self.z, self.h, self.yl, 1 - self.c), device_id_type=MESH,
        ).wait_recv()

    def begin(self):
        for axis in (self.first_axis, "x" if self.first_axis == "z" else "z"):
            self.send(0, 0, axis, 1)
            self.send(0, 0, axis, -1)
            if self.slot < 2 and axis == self.first_axis:
                self.send(0, 0, axis, 2)
                if axis == "z":
                    self.send(0, 0, axis, -2)
        self.send(0, 0, "side", 0)

    def onward(self, dx, dz):
        s = abs(dz)
        if self.first_axis == "z":
            if dx == 0 and self.slot < 2:
                along = {-2: [("z", 1), ("z", 2)], 2: [("z", -1)]}.get(dz, [])
                return along + [("x", 1), ("x", -1)]
            if dx == 0:
                keep = (dz < 0 and s <= 3) or (dz > 0 and s <= 2)
                return ([("z", 1 if dz < 0 else -1)] if keep else []) + [("x", 1), ("x", -1)]
            first = dz % 8 < 4
            return [("x", 1)] if dx == -1 and first else [("x", -1)] if dx == 1 and not first else []
        if dz == 0:
            return ([("x", 1)] if dx == -1 and self.slot > 1 else []) + [("z", 1), ("z", -1)]
        first = dx in (0, 1)
        if dz < 0:
            return [("z", 1)] if s <= 2 or (s == 3 and first) else []
        return [("z", -1)] if s <= 2 or (s == 3 and not first) else []

    def run(self, dx, dz):
        self.arrived(dx, dz)
        for axis, step in self.onward(dx, dz):
            self.send(dx, dz, axis, step)
        self.send(dx, dz, "side", 0)

    def finish_sides(self):
        for dx in range(NX):
            for dz in range(NZ):
                self.arrived(dx, dz, side=True)

    def finish_sends(self):
        for copy in self.sent:
            copy.wait_send()


def main_kernel(
    q_ref, k_ref, v_ref, seg_ref, freq_ref, w_ref, out_ref,
    kin, vin, krot, win, qin, kall, vall, tags, wall, qa, top, norm, acc, acts, obuf, cown, cpart, cgot,
    ring_sem, side_sem, send_sem, act_send, act_recv, in_send, in_recv, cnt_send, cnt_recv, out_send, out_recv,
):
    x, z, h, yl, c = here()
    y = 2 * h + yl
    ci = x * NZ + z
    far = NCHUNK - 1 - ci
    side = ident(x, z, h, yl, 1 - c)
    swap = ident(x, z, c, yl, h)
    flip_swap = ident(NX - 1 - x, NZ - 1 - z, c, yl, h)
    w_dest = ident(2 * yl + h, z, lax.rem(x, 2), x // 2, c)
    keeps = h == c
    keeps_w = x == 2 * yl + h

    def along_y(step):
        there = mod(y + step, 4)
        return ident(x, z, there // 2, lax.rem(there, 2), c)

    def heads_at(step):
        there = mod(y + step, 4)
        return 2 * lax.rem(there, 2) + there // 2

    by_z = [ident(x, mod(z + d, NZ), h, yl, c) for d in range(1, NZ)]
    by_xh = [ident(mod(x + d, NX), z, mod(h + e, 2), yl, c) for d in range(NX) for e in range(2) if d or e]
    barrier = pltpu.get_barrier_semaphore()
    always = by_z + by_xh + [along_y(1), along_y(-1), side, flip_swap, swap, w_dest]
    for peer in always:
        pl.semaphore_signal(barrier, inc=1, device_id=peer, device_id_type=MESH)
    labels = lax.broadcasted_iota(jnp.int32, (BLK, 128), 1)
    own_counts = jnp.sum(jnp.where(seg_ref[...] == labels, 1.0, 0.0), axis=0, keepdims=True)
    cown[...] = jnp.broadcast_to(own_counts, (8, 128)).astype(jnp.int32)
    pl.semaphore_wait(barrier, len(always))

    def remote(slot, source, dest, target, send, recv):
        return pltpu.make_async_remote_copy(
            src_ref=source, dst_ref=dest, send_sem=send.at[slot], recv_sem=recv.at[slot],
            device_id=target, device_id_type=MESH,
        )

    def count_phase(at, source, peers, between):
        copies = [remote(at + i, source, cgot.at[at + i], p, cnt_send, cnt_recv) for i, p in enumerate(peers)]
        for copy in copies:
            copy.start()
        between()
        total = source[...]
        for i, copy in enumerate(copies):
            copy.wait()
            total = total + cgot[at + i]
        return total

    low, high = pl.ds(0, HALF), pl.ds(HALF, HALF)
    moved = {
        "v": (keeps, remote(0, v_ref, vin, swap, in_send, in_recv)),
        "k": (keeps, remote(1, k_ref, kin, swap, in_send, in_recv)),
        "q": (keeps, remote(2, q_ref.at[low], qin.at[low], swap, in_send, in_recv)),
        "w": (keeps_w, remote(3, w_ref, win, w_dest, in_send, in_recv)),
    }
    own_copy = {
        "v": lambda: vin.__setitem__(..., v_ref[...]),
        "k": lambda: kin.__setitem__(..., k_ref[...]),
        "q": lambda: qin.__setitem__((low, slice(None)), q_ref[low, :]),
        "w": lambda: win.__setitem__(..., w_ref[...]),
    }
    upper = remote(4, q_ref.at[high], qin.at[high], flip_swap, in_send, in_recv)

    def start_move(name):
        own, copy = moved[name]
        pl.when(own)(own_copy[name])
        pl.when(jnp.logical_not(own))(copy.start)

    def end_move(name):
        own, copy = moved[name]
        pl.when(jnp.logical_not(own))(copy.wait_recv)

    sems = (ring_sem, side_sem, send_sem)
    plan = Plan()
    a_rows, b_rows = pl.ds(0, WSPLIT), pl.ds(WSPLIT, WROWS - WSPLIT)
    vg = Gather(plan, 0, "x", 48, lambda i, t: vall.at[i, t], vin, *sems)
    kg = Gather(plan, 1, "z", 48, lambda i, t: kall.at[i, t], krot, *sems)
    wa = Gather(plan, 2, "z", WSPLIT / 4, lambda i, t: wall.at[i, t, a_rows], win.at[a_rows], *sems)
    wb = Gather(plan, 3, "x", (WROWS - WSPLIT) / 4, lambda i, t: wall.at[i, t, b_rows], win.at[b_rows], *sems)

    def first_moves():
        start_move("v")
        start_move("k")
        start_move("w")

    def second_moves():
        end_move("v")
        vg.begin()
        vall[ci, c] = vin[...]

    def third_moves():
        start_move("q")
        upper.start()

    cpart[...] = count_phase(0, cown, by_xh, first_moves)
    totals = count_phase(7, cpart, by_z, second_moves)[0:1].astype(jnp.float32)
    third_moves()
    plan.now = 7.0
    lane = lax.broadcasted_iota(jnp.int32, (1, 128), 1)
    ends = totals
    for shift in (1, 2, 4, 8, 16, 32, 64):
        ends = ends + jnp.where(lane >= shift, pltpu.roll(ends, shift, 1), 0.0)
    starts = ends - totals

    def rows_from(first, count):
        return (first + lax.broadcasted_iota(jnp.int32, (count, 128), 0)).astype(jnp.float32)

    def turns(first, count):
        rows = rows_from(first, count)
        start = jnp.max(jnp.where(ends <= rows, ends, 0.0), axis=1, keepdims=True)
        angles = (rows - start) * freq_ref[0:1, :]
        sine = jnp.sin(angles)
        lanes = lax.broadcasted_iota(jnp.int32, (count, 128), 1)
        return jnp.cos(angles), jnp.where(lanes < HEAD_DIM // 2, -sine, sine)

    def rotated(block, cosine, sine):
        wide = block.astype(jnp.float32)
        return (wide * cosine + pltpu.roll(wide, HEAD_DIM // 2, 1) * sine).astype(jnp.bfloat16)

    first_key = ci * CHUNK + c * BLK
    key_cos, key_sin = turns(first_key, BLK)
    end_move("k")
    krot[...] = rotated(kin[...], key_cos, key_sin)
    kg.begin()
    kall[ci, c] = krot[...]
    plan.poll(0.3)
    top[...] = jnp.full(top.shape, BIG, jnp.float32)
    norm[...] = jnp.zeros_like(norm)
    acc[...] = jnp.zeros_like(acc)
    plan.poll(0.4)

    def inside(rows):
        return (rows >= starts) & (rows < ends)

    def tag(i, carry):
        tags[i] = jnp.where(inside(rows_from(i * CHUNK, CHUNK)), 1.0, 0.0).astype(jnp.bfloat16)
        return carry

    lax.fori_loop(0, NCHUNK, tag, 0)
    plan.poll(1.6)
    up_cos, up_sin = turns(far * CHUNK + c * BLK + HALF, HALF)
    upper.wait_recv()
    end_move("q")
    for half, (cosine, sine) in enumerate(((key_cos[:HALF], key_sin[:HALF]), (up_cos, up_sin))):
        rows = pl.ds(half * HALF, HALF)
        first_row = ci * CHUNK + c * BLK if half == 0 else far * CHUNK + c * BLK + HALF
        lanes = lax.broadcasted_iota(jnp.int32, (HALF, 128), 1)
        hidden = jnp.logical_not(inside(rows_from(first_row, HALF))) & (lanes < SEGMENTS)
        penalty = jnp.where(hidden, BIG, 0.0).astype(jnp.bfloat16)
        for head in range(GROUP):
            at = pl.ds(head * HALF, HALF)
            qa[half, at, 0:HEAD_DIM] = rotated(qin[rows, head * HEAD_DIM : (head + 1) * HEAD_DIM], cosine, sine)
            qa[half, at, HEAD_DIM : 2 * HEAD_DIM] = penalty
    plan.poll(0.5)
    plan.held = True
    end_move("w")
    wa.begin()
    wb.begin()
    wall[ci, c] = win[...]
    plan.until(vg.keys() + kg.keys())
    plan.release()
    kg.finish_sides()
    vg.finish_sides()

    factor = math.log2(math.e) / math.sqrt(HEAD_DIM)

    def attend(half, chunk, mask_from=None):
        keys = jnp.concatenate([kall[chunk].reshape(CHUNK, HEAD_DIM), tags[chunk]], axis=1)
        vals = vall[chunk].reshape(CHUNK, HEAD_DIM)
        size = GROUP * HALF // 2
        tiles = [pl.ds(r, size) for r in range(0, GROUP * HALF, size)]
        olds = [(top[half, r], norm[half, r], acc[half, r]) for r in tiles]

        def scored(r):
            found = lax.dot_general(
                qa[half, r], keys, (((1,), (1,)), ((), ())), preferred_element_type=jnp.float32
            )
            if mask_from is not None:
                row = lax.rem(lax.broadcasted_iota(jnp.int32, found.shape, 0), HALF) + mask_from
                column = chunk * CHUNK + lax.broadcasted_iota(jnp.int32, found.shape, 1)
                found = jnp.where(column <= row, found, BIG)
            return found

        ahead = scored(tiles[0])
        news = []
        for n in range(len(tiles)):
            scores = ahead
            if n + 1 < len(tiles):
                ahead = scored(tiles[n + 1])
            before, total, mix = olds[n]
            peak = jnp.maximum(before, jnp.max(scores, axis=1, keepdims=True))
            fade = jnp.exp2((before - peak) * factor)
            parts = [jnp.exp2((scores[:, i : i + 128] - peak) * factor) for i in range(0, CHUNK, 128)]
            weights = jnp.concatenate([p.astype(jnp.bfloat16) for p in parts], axis=1)
            added = jnp.dot(weights, vals, preferred_element_type=jnp.float32)
            news.append((peak, total * fade + sum(parts[1:], parts[0]), mix * fade + added))
        for r, (a, b, d) in zip(tiles, news):
            top[half, r] = a
            norm[half, r] = b
            acc[half, r] = d

    early = jnp.where(ci < far, 0, 1)
    n_early = jnp.minimum(ci, far)

    def step(i, carry):
        is_early = i < n_early
        attend(jnp.where(is_early, early, 1 - early), jnp.where(is_early, i, i - n_early))
        return carry

    def steps(lo, hi):
        lax.fori_loop(lo, hi, step, 0)
        plan.poll(0.6 * (hi - lo))

    mine = heads_at(0)
    below, above, far_heads = heads_at(-1), heads_at(1), heads_at(2)
    act_copies = []

    def act_start(slot, part, rows, along, key, arrive):
        copy = remote(slot, acts.at[part, rows], acts.at[part, rows], along_y(along), act_send, act_recv)
        copy.start()
        act_copies.append(copy)
        plan.sent(("y", along), 192, key, lambda: arrive(copy))

    def spread(n, half):
        total = jnp.sum(norm[half], axis=1, keepdims=True)
        result = (acc[half] / total).astype(jnp.bfloat16)
        rows = pl.ds(pl.multiple_of(half * HALF, HALF), HALF)
        for head in range(GROUP):
            acts[mine, rows, head * HEAD_DIM : (head + 1) * HEAD_DIM] = result[head * HALF : (head + 1) * HALF]

        def landed(copy):
            copy.wait_recv()

        def onward(copy):
            copy.wait_recv()
            part, along = (below, 1) if n == 0 else (above, -1)
            act_start(3 * n + 2, part, rows, along, ("a", n, 2), landed)

        act_start(3 * n, mine, rows, 1, ("a", n, 0), onward if n == 0 else landed)
        act_start(3 * n + 1, mine, rows, -1, ("a", n, 1), landed if n == 0 else onward)
        plan.poll(0.3)

    attend(0, ci, ci * CHUNK + c * BLK)
    plan.poll(0.7)
    attend(1, far, far * CHUNK + c * BLK + HALF)
    plan.poll(0.7)
    for lo in range(0, 16, 2):
        steps(lo, lo + 2)
    spread(0, early)
    for lo in range(16, 31, 2):
        steps(lo, min(lo + 2, 31))
    spread(1, 1 - early)
    plan.until([("a", n, i) for n in range(2) for i in range(3)])

    given = []
    for dz in ORDER:
        zi = mod(z + dz, NZ)
        plan.until([g.key(dx, dz) for g in (wa, wb) for dx in range(NX) if dx or dz])
        for dx in (0, -1, 1, 2):
            wa.arrived(dx, dz, side=True)
            wb.arrived(dx, dz, side=True)
        total = jnp.zeros((BLK, 256), jnp.float32)
        for kk in range(NX):
            pair = [wall[(2 * (kk // 2) + t) * NZ + zi, kk % 2] for t in range(2)]
            total = total + jnp.dot(acts[kk], jnp.concatenate(pair, axis=1), preferred_element_type=jnp.float32)
        block = total.astype(jnp.bfloat16)
        lower_copy = remote(zi, obuf.at[zi, low], out_ref.at[zi, low], swap, out_send, out_recv)
        upper_copy = remote(NZ + zi, obuf.at[zi, high], out_ref.at[zi, high], flip_swap, out_send, out_recv)
        given.append((lower_copy, upper_copy))
        obuf[zi] = block
        upper_copy.start()

        @pl.when(keeps)
        def _(zi=zi, block=block):
            out_ref[zi, 0:HALF] = block[0:HALF]

        pl.when(jnp.logical_not(keeps))(lower_copy.start)
        plan.poll(1.0)

    for g in (vg, kg, wa, wb):
        g.finish_sends()
    for copy in act_copies:
        copy.wait_send()
    upper.wait_send()
    for own, copy in moved.values():
        pl.when(jnp.logical_not(own))(copy.wait_send)

    for lower_copy, upper_copy in given:
        upper_copy.wait()
        pl.when(jnp.logical_not(keeps))(lower_copy.wait)


def main_call(q, k, v, seg, freq, w):
    rows = GROUP * HALF
    return pl.pallas_call(
        main_kernel,
        out_shape=jax.ShapeDtypeStruct((NZ, BLK, 256), jnp.bfloat16),
        in_specs=[pl.BlockSpec(memory_space=pltpu.VMEM)] * 6,
        out_specs=pl.BlockSpec(memory_space=pltpu.VMEM),
        scratch_shapes=[
            pltpu.VMEM((BLK, HEAD_DIM), jnp.bfloat16),
            pltpu.VMEM((BLK, HEAD_DIM), jnp.bfloat16),
            pltpu.VMEM((BLK, HEAD_DIM), jnp.bfloat16),
            pltpu.VMEM((WROWS, 128), jnp.bfloat16),
            pltpu.VMEM((BLK, GROUP * HEAD_DIM), jnp.bfloat16),
            pltpu.VMEM((NCHUNK, 2, BLK, HEAD_DIM), jnp.bfloat16),
            pltpu.VMEM((NCHUNK, 2, BLK, HEAD_DIM), jnp.bfloat16),
            pltpu.VMEM((NCHUNK, CHUNK, 128), jnp.bfloat16),
            pltpu.VMEM((NCHUNK, 2, WROWS, 128), jnp.bfloat16),
            pltpu.VMEM((2, rows, 2 * HEAD_DIM), jnp.bfloat16),
            pltpu.VMEM((2, rows, 128), jnp.float32),
            pltpu.VMEM((2, rows, 128), jnp.float32),
            pltpu.VMEM((2, rows, HEAD_DIM), jnp.float32),
            pltpu.VMEM((4, BLK, GROUP * HEAD_DIM), jnp.bfloat16),
            pltpu.VMEM((NZ, BLK, 256), jnp.bfloat16),
            pltpu.VMEM((8, 128), jnp.int32),
            pltpu.VMEM((8, 128), jnp.int32),
            pltpu.VMEM((14, 8, 128), jnp.int32),
            pltpu.SemaphoreType.DMA((4, NCHUNK)),
            pltpu.SemaphoreType.DMA((4, NCHUNK)),
            pltpu.SemaphoreType.DMA((4, 64)),
            pltpu.SemaphoreType.DMA((6,)),
            pltpu.SemaphoreType.DMA((6,)),
            pltpu.SemaphoreType.DMA((5,)),
            pltpu.SemaphoreType.DMA((5,)),
            pltpu.SemaphoreType.DMA((14,)),
            pltpu.SemaphoreType.DMA((14,)),
            pltpu.SemaphoreType.DMA((2 * NZ,)),
            pltpu.SemaphoreType.DMA((2 * NZ,)),
        ],
        compiler_params=pltpu.CompilerParams(
            collective_id=2, has_side_effects=True, vmem_limit_bytes=60 * 1024 * 1024
        ),
        name="attend_project",
    )(q, k, v, seg, freq, w)


def local(queries, keys, values, segment_ids, out_weight):
    half_dim = HEAD_DIM // 2
    exponent = jnp.arange(half_dim, dtype=jnp.float32) * (2.0 / HEAD_DIM)
    inverse = jnp.power(jnp.float32(ROPE_BASE), -exponent)
    freq = jnp.broadcast_to(jnp.concatenate([inverse, inverse])[None, :], (8, HEAD_DIM))
    segments = jnp.broadcast_to(segment_ids[:, None], (BLK, 128))
    tile = main_call(queries, keys, values, segments, freq, out_weight)
    return jnp.transpose(tile, (1, 0, 2)).reshape(BLK, NZ * 256)


def solution(mesh):
    return jax.shard_map(
        local,
        mesh=mesh,
        in_specs=(P("seq", "tp"), P("seq", "tp"), P("seq", "tp"), P("seq"), P("tp", "seq")),
        out_specs=P("seq", "tp"),
        check_vma=False,
    )
```

```python
import functools
import math

import jax
import jax.numpy as jnp
from jax import lax
from jax.experimental import pallas as pl
from jax.experimental.pallas import tpu as pltpu
from jax.sharding import PartitionSpec as P

HEAD_DIM = 128
SEGMENTS = 16
NX, NZ = 4, 8
BLK = 192
HALF = 96
GROUP = 8
CHUNK = 384
NCHUNK = 32
WROWS = 1024
WSPLIT = 560
ROPE_BASE = 500000.0
BIG = -1e30
MESH = pl.DeviceIdType.MESH


def coords(j, k):
    return j // 16, (j // 2) % 8, j % 2, k // 2, k % 2


def seq_tp(x, z, h, yl, c):
    return x * 16 + z * 2 + h, yl * 2 + c


def here():
    j = lax.axis_index("seq")
    k = lax.axis_index("tp")
    return coords(j, k)


def ident(x, z, h, yl, c):
    return {"seq": x * 16 + z * 2 + h, "tp": yl * 2 + c}


def plane_shift(y, c):
    return jnp.where(y == 2, 2, jnp.where(y == 0, 0, jnp.where((y == 1) == (c == 0), 1, 3)))


def shift_of(y, c):
    return y if y % 2 == 0 else 1 if (y == 1) == (c == 0) else 3


def mod(value, n):
    return lax.rem(value + 2 * n, n)


ORDER = (0, -1, 1, -2, 2, -3, 3, -4)
LINK_KB_PER_US = 40.0
HOP_US = 2.2


class Plan:
    def __init__(self):
        self.put_off = []
        self.now, self.free, self.events, self.done, self.held = 0.0, {}, [], set(), False

    def sent(self, link, size, key, arrive):
        start = max(self.now, self.free.get(link, 0.0))
        self.free[link] = start + size / LINK_KB_PER_US
        self.events.append((self.free[link] + HOP_US, len(self.events), key, arrive))

    def take(self, event):
        self.events = [e if e is not event else (1e9, e[1], None, None) for e in self.events]
        self.now = max(self.now, event[0]) + 0.03
        self.done.add(event[2])
        event[3]()
        if self.held:
            self.trickle()

    def late(self, key):
        return (key[0] == 2 and key[1] != 0) or (key[0] == 3 and key[2] != 0)

    def release(self):
        self.held = False
        for _, again in self.put_off:
            again()
        self.put_off = []
        self.poll()

    def trickle(self):
        for item in list(self.put_off):
            if self.free.get(item[0], 0.0) <= self.now:
                self.put_off.remove(item)
                item[1]()

    def first(self):
        return min((e for e in self.events if e[2] and not (self.held and self.late(e[2]))), default=(1e9, 0, None, None))

    def poll(self, spent=0.0):
        self.now += spent
        while self.first()[0] <= self.now - 0.5:
            self.take(self.first())

    def until(self, keys):
        while not set(keys) <= self.done:
            self.take(self.first())


class Gather:
    def __init__(self, plan, slot, first_axis, size, place, own, ring_sem, side_sem, send_sem):
        self.plan, self.slot, self.first_axis, self.size, self.place, self.own = plan, slot, first_axis, size, place, own
        self.ring_sem, self.side_sem, self.send_sem = ring_sem, side_sem, send_sem
        self.sent = []
        self.x, self.z, self.h, self.yl, self.c = here()

    def key(self, dx, dz):
        return self.slot, dx % NX, dz % NZ

    def keys(self):
        return [self.key(dx, dz) for dx in range(NX) for dz in range(NZ) if dx or dz]

    def chunk(self, dx, dz):
        return mod(self.x + dx, NX) * NZ + mod(self.z + dz, NZ)

    def send(self, dx, dz, axis, step, granted=False):
        if self.plan.held and self.slot > 1 and axis not in ("side", self.first_axis) and not granted:
            self.plan.put_off.append(((axis, step), lambda: self.send(dx, dz, axis, step, True)))
            return
        ci = self.chunk(dx, dz)
        there = self.place(ci, self.c)
        source = self.own if (dx, dz) == (0, 0) else there
        recv = self.side_sem if axis == "side" else self.ring_sem
        if axis == "side":
            target = ident(self.x, self.z, self.h, self.yl, 1 - self.c)
        elif axis == "x":
            target = ident(mod(self.x + step, NX), self.z, self.h, self.yl, self.c)
        else:
            target = ident(self.x, mod(self.z + step, NZ), self.h, self.yl, self.c)
        copy = pltpu.make_async_remote_copy(
            src_ref=source, dst_ref=there, send_sem=self.send_sem.at[self.slot, len(self.sent)],
            recv_sem=recv.at[self.slot, ci], device_id=target, device_id_type=MESH,
        )
        copy.start()
        self.sent.append(copy)
        if axis != "side":
            seen = (dx - step, dz) if axis == "x" else (dx, dz - step)
            seen = (2 if seen[0] == -2 else seen[0], seen[1])
            self.plan.sent((axis, 1 if step > 0 else -1), self.size * abs(step), self.key(*seen), lambda: self.run(*seen))

    def arrived(self, dx, dz, side=False):
        ci = self.chunk(dx, dz)
        sem = self.side_sem if side else self.ring_sem
        ref = self.place(ci, 1 - self.c if side else self.c)
        pltpu.make_async_remote_copy(
            src_ref=ref, dst_ref=ref, send_sem=self.send_sem.at[self.slot, 0], recv_sem=sem.at[self.slot, ci],
            device_id=ident(self.x, self.z, self.h, self.yl, 1 - self.c), device_id_type=MESH,
        ).wait_recv()

    def begin(self):
        for axis in (self.first_axis, "x" if self.first_axis == "z" else "z"):
            self.send(0, 0, axis, 1)
            self.send(0, 0, axis, -1)
            if self.slot < 2 and axis == self.first_axis:
                self.send(0, 0, axis, 2)
                if axis == "z":
                    self.send(0, 0, axis, -2)
        self.send(0, 0, "side", 0)

    def onward(self, dx, dz):
        s = abs(dz)
        if self.first_axis == "z":
            if dx == 0 and self.slot < 2:
                along = {-2: [("z", 1), ("z", 2)], 2: [("z", -1)]}.get(dz, [])
                return along + [("x", 1), ("x", -1)]
            if dx == 0:
                keep = (dz < 0 and s <= 3) or (dz > 0 and s <= 2)
                return ([("z", 1 if dz < 0 else -1)] if keep else []) + [("x", 1), ("x", -1)]
            first = dz % 8 < 4
            return [("x", 1)] if dx == -1 and first else [("x", -1)] if dx == 1 and not first else []
        if dz == 0:
            return ([("x", 1)] if dx == -1 and self.slot > 1 else []) + [("z", 1), ("z", -1)]
        first = dx in (0, 1)
        if dz < 0:
            return [("z", 1)] if s <= 2 or (s == 3 and first) else []
        return [("z", -1)] if s <= 2 or (s == 3 and not first) else []

    def run(self, dx, dz):
        self.arrived(dx, dz)
        for axis, step in self.onward(dx, dz):
            self.send(dx, dz, axis, step)
        self.send(dx, dz, "side", 0)

    def finish_sides(self):
        for dx in range(NX):
            for dz in range(NZ):
                self.arrived(dx, dz, side=True)

    def finish_sends(self):
        for copy in self.sent:
            copy.wait_send()


def main_kernel(
    q_ref, k_ref, v_ref, seg_ref, freq_ref, w_ref, out_ref,
    kin, vin, krot, win, qin, kall, vall, tags, wall, qa, top, norm, acc, acts, obuf, cown, cpart, cgot,
    ring_sem, side_sem, send_sem, act_send, act_recv, in_send, in_recv, cnt_send, cnt_recv, out_send, out_recv,
):
    x, z, h, yl, c = here()
    y = 2 * h + yl
    ci = x * NZ + z
    far = NCHUNK - 1 - ci
    side = ident(x, z, h, yl, 1 - c)
    swap = ident(x, z, c, yl, h)
    flip_swap = ident(NX - 1 - x, NZ - 1 - z, c, yl, h)
    w_dest = ident(mod(x + plane_shift(y, c), NX), z, lax.rem(x, 2), x // 2, c)
    plane = 2 * yl + h
    away = mod(x - plane, NX)
    from_y = jnp.where(away == 1, jnp.where(c == 0, 1, 3), jnp.where(away == 3, jnp.where(c == 0, 3, 1), away))
    w_source = ident(plane, z, from_y // 2, lax.rem(from_y, 2), c)
    keeps = h == c
    keeps_w = (mod(x + plane_shift(y, c), NX) == x) & (2 * lax.rem(x, 2) + x // 2 == y)

    def along_y(step):
        there = mod(y + step, 4)
        return ident(x, z, there // 2, lax.rem(there, 2), c)

    def heads_at(step):
        there = mod(y + step, 4)
        return 2 * lax.rem(there, 2) + there // 2

    by_z = [ident(x, mod(z + d, NZ), h, yl, c) for d in range(1, NZ)]
    by_xh = [ident(mod(x + d, NX), z, mod(h + e, 2), yl, c) for d in range(NX) for e in range(2) if d or e]
    barrier = pltpu.get_barrier_semaphore()
    always = by_z + by_xh + [along_y(1), along_y(-1), side, flip_swap, swap, w_dest, w_source]
    for peer in always:
        pl.semaphore_signal(barrier, inc=1, device_id=peer, device_id_type=MESH)
    labels = lax.broadcasted_iota(jnp.int32, (BLK, 128), 1)
    own_counts = jnp.sum(jnp.where(seg_ref[...] == labels, 1.0, 0.0), axis=0, keepdims=True)
    cown[...] = jnp.broadcast_to(own_counts, (8, 128)).astype(jnp.int32)
    pl.semaphore_wait(barrier, len(always))

    def remote(slot, source, dest, target, send, recv):
        return pltpu.make_async_remote_copy(
            src_ref=source, dst_ref=dest, send_sem=send.at[slot], recv_sem=recv.at[slot],
            device_id=target, device_id_type=MESH,
        )

    def count_phase(at, source, peers, between):
        copies = [remote(at + i, source, cgot.at[at + i], p, cnt_send, cnt_recv) for i, p in enumerate(peers)]
        for copy in copies:
            copy.start()
        between()
        total = source[...]
        for i, copy in enumerate(copies):
            copy.wait()
            total = total + cgot[at + i]
        return total

    low, high = pl.ds(0, HALF), pl.ds(HALF, HALF)
    moved = {
        "v": (keeps, remote(0, v_ref, vin, swap, in_send, in_recv)),
        "k": (keeps, remote(1, k_ref, kin, swap, in_send, in_recv)),
        "q": (keeps, remote(2, q_ref.at[low], qin.at[low], swap, in_send, in_recv)),
        "w": (keeps_w, remote(3, w_ref, win, w_dest, in_send, in_recv)),
    }
    own_copy = {
        "v": lambda: vin.__setitem__(..., v_ref[...]),
        "k": lambda: kin.__setitem__(..., k_ref[...]),
        "q": lambda: qin.__setitem__((low, slice(None)), q_ref[low, :]),
        "w": lambda: win.__setitem__(..., w_ref[...]),
    }
    upper = remote(4, q_ref.at[high], qin.at[high], flip_swap, in_send, in_recv)

    def start_move(name):
        own, copy = moved[name]
        pl.when(own)(own_copy[name])
        pl.when(jnp.logical_not(own))(copy.start)

    def end_move(name):
        own, copy = moved[name]
        pl.when(jnp.logical_not(own))(copy.wait_recv)

    sems = (ring_sem, side_sem, send_sem)
    plan = Plan()
    a_rows, b_rows = pl.ds(0, WSPLIT), pl.ds(WSPLIT, WROWS - WSPLIT)
    vg = Gather(plan, 0, "z", 48, lambda i, t: vall.at[i, t], vin, *sems)
    kg = Gather(plan, 1, "x", 48, lambda i, t: kall.at[i, t], krot, *sems)
    wa = Gather(plan, 2, "z", WSPLIT / 4, lambda i, t: wall.at[i, t, a_rows], win.at[a_rows], *sems)
    wb = Gather(plan, 3, "x", (WROWS - WSPLIT) / 4, lambda i, t: wall.at[i, t, b_rows], win.at[b_rows], *sems)

    def first_moves():
        start_move("v")
        start_move("k")
        start_move("w")

    def second_moves():
        end_move("v")
        vg.begin()
        vall[ci, c] = vin[...]

    def third_moves():
        start_move("q")
        upper.start()

    cpart[...] = count_phase(0, cown, by_xh, first_moves)
    totals = count_phase(7, cpart, by_z, second_moves)[0:1].astype(jnp.float32)
    third_moves()
    plan.now = 7.0
    lane = lax.broadcasted_iota(jnp.int32, (1, 128), 1)
    ends = totals
    for shift in (1, 2, 4, 8, 16, 32, 64):
        ends = ends + jnp.where(lane >= shift, pltpu.roll(ends, shift, 1), 0.0)
    starts = ends - totals

    def rows_from(first, count):
        return (first + lax.broadcasted_iota(jnp.int32, (count, 128), 0)).astype(jnp.float32)

    def turns(first, count):
        rows = rows_from(first, count)
        start = jnp.max(jnp.where(ends <= rows, ends, 0.0), axis=1, keepdims=True)
        angles = (rows - start) * freq_ref[0:1, :]
        sine = jnp.sin(angles)
        lanes = lax.broadcasted_iota(jnp.int32, (count, 128), 1)
        return jnp.cos(angles), jnp.where(lanes < HEAD_DIM // 2, -sine, sine)

    def rotated(block, cosine, sine):
        wide = block.astype(jnp.float32)
        return (wide * cosine + pltpu.roll(wide, HEAD_DIM // 2, 1) * sine).astype(jnp.bfloat16)

    first_key = ci * CHUNK + c * BLK
    key_cos, key_sin = turns(first_key, BLK)
    end_move("k")
    krot[...] = rotated(kin[...], key_cos, key_sin)
    kg.begin()
    kall[ci, c] = krot[...]
    plan.poll(0.3)
    top[...] = jnp.full(top.shape, BIG, jnp.float32)
    norm[...] = jnp.zeros_like(norm)
    acc[...] = jnp.zeros_like(acc)
    plan.poll(0.4)

    def inside(rows):
        return (rows >= starts) & (rows < ends)

    def tag(i, carry):
        tags[i] = jnp.where(inside(rows_from(i * CHUNK, CHUNK)), 1.0, 0.0).astype(jnp.bfloat16)
        return carry

    lax.fori_loop(0, NCHUNK, tag, 0)
    plan.poll(1.6)
    plan.held = True
    plan.until([vg.key(0, dz) for dz in (1, -1)] + [kg.key(dx, 0) for dx in (1, -1)])
    end_move("w")
    wa.begin()
    wb.begin()
    wall[ci, c] = win[...]
    plan.until(vg.keys() + kg.keys())
    up_cos, up_sin = turns(far * CHUNK + c * BLK + HALF, HALF)
    upper.wait_recv()
    end_move("q")
    for half, (cosine, sine) in enumerate(((key_cos[:HALF], key_sin[:HALF]), (up_cos, up_sin))):
        rows = pl.ds(half * HALF, HALF)
        first_row = ci * CHUNK + c * BLK if half == 0 else far * CHUNK + c * BLK + HALF
        lanes = lax.broadcasted_iota(jnp.int32, (HALF, 128), 1)
        hidden = jnp.logical_not(inside(rows_from(first_row, HALF))) & (lanes < SEGMENTS)
        penalty = jnp.where(hidden, BIG, 0.0).astype(jnp.bfloat16)
        for head in range(GROUP):
            at = pl.ds(head * HALF, HALF)
            qa[half, at, 0:HEAD_DIM] = rotated(qin[rows, head * HEAD_DIM : (head + 1) * HEAD_DIM], cosine, sine)
            qa[half, at, HEAD_DIM : 2 * HEAD_DIM] = penalty
    plan.release()
    kg.finish_sides()
    vg.finish_sides()

    factor = math.log2(math.e) / math.sqrt(HEAD_DIM)

    def attend(half, chunk, mask_from=None):
        keys = jnp.concatenate([kall[chunk].reshape(CHUNK, HEAD_DIM), tags[chunk]], axis=1)
        vals = vall[chunk].reshape(CHUNK, HEAD_DIM)
        size = GROUP * HALF // 2
        tiles = [pl.ds(r, size) for r in range(0, GROUP * HALF, size)]
        olds = [(top[half, r], norm[half, r], acc[half, r]) for r in tiles]

        def scored(r):
            found = lax.dot_general(
                qa[half, r], keys, (((1,), (1,)), ((), ())), preferred_element_type=jnp.float32
            )
            if mask_from is not None:
                row = lax.rem(lax.broadcasted_iota(jnp.int32, found.shape, 0), HALF) + mask_from
                column = chunk * CHUNK + lax.broadcasted_iota(jnp.int32, found.shape, 1)
                found = jnp.where(column <= row, found, BIG)
            return found

        ahead = scored(tiles[0])
        news = []
        for n in range(len(tiles)):
            scores = ahead
            if n + 1 < len(tiles):
                ahead = scored(tiles[n + 1])
            before, total, mix = olds[n]
            peak = jnp.maximum(before, jnp.max(scores, axis=1, keepdims=True))
            fade = jnp.exp2((before - peak) * factor)
            parts = [jnp.exp2((scores[:, i : i + 128] - peak) * factor) for i in range(0, CHUNK, 128)]
            weights = jnp.concatenate([p.astype(jnp.bfloat16) for p in parts], axis=1)
            added = jnp.dot(weights, vals, preferred_element_type=jnp.float32)
            news.append((peak, total * fade + sum(parts[1:], parts[0]), mix * fade + added))
        for r, (a, b, d) in zip(tiles, news):
            top[half, r] = a
            norm[half, r] = b
            acc[half, r] = d

    early = jnp.where(ci < far, 0, 1)
    n_early = jnp.minimum(ci, far)

    def step(i, carry):
        is_early = i < n_early
        attend(jnp.where(is_early, early, 1 - early), jnp.where(is_early, i, i - n_early))
        return carry

    def steps(lo, hi):
        lax.fori_loop(lo, hi, step, 0)
        plan.poll(0.6 * (hi - lo))

    mine = heads_at(0)
    below, above, far_heads = heads_at(-1), heads_at(1), heads_at(2)
    act_copies = []

    def act_start(slot, part, rows, along, key, arrive):
        copy = remote(slot, acts.at[part, rows], acts.at[part, rows], along_y(along), act_send, act_recv)
        copy.start()
        act_copies.append(copy)
        plan.sent(("y", along), 192, key, lambda: arrive(copy))

    def spread(n, half):
        total = jnp.sum(norm[half], axis=1, keepdims=True)
        result = (acc[half] / total).astype(jnp.bfloat16)
        rows = pl.ds(pl.multiple_of(half * HALF, HALF), HALF)
        for head in range(GROUP):
            acts[mine, rows, head * HEAD_DIM : (head + 1) * HEAD_DIM] = result[head * HALF : (head + 1) * HALF]

        def landed(copy):
            copy.wait_recv()

        def onward(copy):
            copy.wait_recv()
            part, along = (below, 1) if n == 0 else (above, -1)
            act_start(3 * n + 2, part, rows, along, ("a", n, 2), landed)

        act_start(3 * n, mine, rows, 1, ("a", n, 0), onward if n == 0 else landed)
        act_start(3 * n + 1, mine, rows, -1, ("a", n, 1), landed if n == 0 else onward)
        plan.poll(0.3)

    attend(0, ci, ci * CHUNK + c * BLK)
    plan.poll(0.7)
    attend(1, far, far * CHUNK + c * BLK + HALF)
    plan.poll(0.7)
    for lo in range(0, 16, 2):
        steps(lo, lo + 2)
    spread(0, early)
    for lo in range(16, 31, 2):
        steps(lo, min(lo + 2, 31))
    spread(1, 1 - early)
    plan.until([("a", n, i) for n in range(2) for i in range(3)])

    given = []
    for dz in ORDER:
        zi = mod(z + dz, NZ)
        plan.until([g.key(dx, dz) for g in (wa, wb) for dx in range(NX) if dx or dz])
        for dx in (0, -1, 1, 2):
            wa.arrived(dx, dz, side=True)
            wb.arrived(dx, dz, side=True)
        total = jnp.zeros((BLK, 256), jnp.float32)
        for kk in range(NX):
            pair = [wall[mod(plane + shift_of(2 * t + kk // 2, kk % 2), NX) * NZ + zi, kk % 2] for t in range(2)]
            total = total + jnp.dot(acts[kk], jnp.concatenate(pair, axis=1), preferred_element_type=jnp.float32)
        block = total.astype(jnp.bfloat16)
        lower_copy = remote(zi, obuf.at[zi, low], out_ref.at[zi, low], swap, out_send, out_recv)
        upper_copy = remote(NZ + zi, obuf.at[zi, high], out_ref.at[zi, high], flip_swap, out_send, out_recv)
        given.append((lower_copy, upper_copy))
        obuf[zi] = block
        upper_copy.start()

        @pl.when(keeps)
        def _(zi=zi, block=block):
            out_ref[zi, 0:HALF] = block[0:HALF]

        pl.when(jnp.logical_not(keeps))(lower_copy.start)
        plan.poll(1.0)

    for g in (vg, kg, wa, wb):
        g.finish_sends()
    for copy in act_copies:
        copy.wait_send()
    upper.wait_send()
    for own, copy in moved.values():
        pl.when(jnp.logical_not(own))(copy.wait_send)

    for lower_copy, upper_copy in given:
        upper_copy.wait()
        pl.when(jnp.logical_not(keeps))(lower_copy.wait)


def main_call(q, k, v, seg, freq, w):
    rows = GROUP * HALF
    return pl.pallas_call(
        main_kernel,
        out_shape=jax.ShapeDtypeStruct((NZ, BLK, 256), jnp.bfloat16),
        in_specs=[pl.BlockSpec(memory_space=pltpu.VMEM)] * 6,
        out_specs=pl.BlockSpec(memory_space=pltpu.VMEM),
        scratch_shapes=[
            pltpu.VMEM((BLK, HEAD_DIM), jnp.bfloat16),
            pltpu.VMEM((BLK, HEAD_DIM), jnp.bfloat16),
            pltpu.VMEM((BLK, HEAD_DIM), jnp.bfloat16),
            pltpu.VMEM((WROWS, 128), jnp.bfloat16),
            pltpu.VMEM((BLK, GROUP * HEAD_DIM), jnp.bfloat16),
            pltpu.VMEM((NCHUNK, 2, BLK, HEAD_DIM), jnp.bfloat16),
            pltpu.VMEM((NCHUNK, 2, BLK, HEAD_DIM), jnp.bfloat16),
            pltpu.VMEM((NCHUNK, CHUNK, 128), jnp.bfloat16),
            pltpu.VMEM((NCHUNK, 2, WROWS, 128), jnp.bfloat16),
            pltpu.VMEM((2, rows, 2 * HEAD_DIM), jnp.bfloat16),
            pltpu.VMEM((2, rows, 128), jnp.float32),
            pltpu.VMEM((2, rows, 128), jnp.float32),
            pltpu.VMEM((2, rows, HEAD_DIM), jnp.float32),
            pltpu.VMEM((4, BLK, GROUP * HEAD_DIM), jnp.bfloat16),
            pltpu.VMEM((NZ, BLK, 256), jnp.bfloat16),
            pltpu.VMEM((8, 128), jnp.int32),
            pltpu.VMEM((8, 128), jnp.int32),
            pltpu.VMEM((14, 8, 128), jnp.int32),
            pltpu.SemaphoreType.DMA((4, NCHUNK)),
            pltpu.SemaphoreType.DMA((4, NCHUNK)),
            pltpu.SemaphoreType.DMA((4, 64)),
            pltpu.SemaphoreType.DMA((6,)),
            pltpu.SemaphoreType.DMA((6,)),
            pltpu.SemaphoreType.DMA((5,)),
            pltpu.SemaphoreType.DMA((5,)),
            pltpu.SemaphoreType.DMA((14,)),
            pltpu.SemaphoreType.DMA((14,)),
            pltpu.SemaphoreType.DMA((2 * NZ,)),
            pltpu.SemaphoreType.DMA((2 * NZ,)),
        ],
        compiler_params=pltpu.CompilerParams(
            collective_id=2, has_side_effects=True, vmem_limit_bytes=60 * 1024 * 1024
        ),
        name="attend_project",
    )(q, k, v, seg, freq, w)


def local(queries, keys, values, segment_ids, out_weight):
    half_dim = HEAD_DIM // 2
    exponent = jnp.arange(half_dim, dtype=jnp.float32) * (2.0 / HEAD_DIM)
    inverse = jnp.power(jnp.float32(ROPE_BASE), -exponent)
    freq = jnp.broadcast_to(jnp.concatenate([inverse, inverse])[None, :], (8, HEAD_DIM))
    segments = jnp.broadcast_to(segment_ids[:, None], (BLK, 128))
    tile = main_call(queries, keys, values, segments, freq, out_weight)
    return jnp.transpose(tile, (1, 0, 2)).reshape(BLK, NZ * 256)


def solution(mesh):
    return jax.shard_map(
        local,
        mesh=mesh,
        in_specs=(P("seq", "tp"), P("seq", "tp"), P("seq", "tp"), P("seq"), P("tp", "seq")),
        out_specs=P("seq", "tp"),
        check_vma=False,
    )
```

```python
import functools
import math

import jax
import jax.numpy as jnp
from jax import lax
from jax.experimental import pallas as pl
from jax.experimental.pallas import tpu as pltpu
from jax.sharding import PartitionSpec as P

HEAD_DIM = 128
SEGMENTS = 16
NX, NZ = 4, 8
BLK = 192
HALF = 96
GROUP = 8
CHUNK = 384
NCHUNK = 32
WROWS = 1024
WSPLIT = 560
ROPE_BASE = 500000.0
BIG = -1e30
MESH = pl.DeviceIdType.MESH


def coords(j, k):
    return j // 16, (j // 2) % 8, j % 2, k // 2, k % 2


def seq_tp(x, z, h, yl, c):
    return x * 16 + z * 2 + h, yl * 2 + c


def here():
    j = lax.axis_index("seq")
    k = lax.axis_index("tp")
    return coords(j, k)


def ident(x, z, h, yl, c):
    return {"seq": x * 16 + z * 2 + h, "tp": yl * 2 + c}


def plane_shift(y, c):
    return jnp.where(y == 2, 2, jnp.where(y == 0, 0, jnp.where((y == 1) == (c == 0), 1, 3)))


def shift_of(y, c):
    return y if y % 2 == 0 else 1 if (y == 1) == (c == 0) else 3


def mod(value, n):
    return lax.rem(value + 2 * n, n)


ORDER = (0, -1, 1, -2, 2, -3, 3, -4)
LINK_KB_PER_US = 40.0
HOP_US = 2.2


class Plan:
    def __init__(self):
        self.put_off = []
        self.now, self.free, self.events, self.done, self.held = 0.0, {}, [], set(), False

    def sent(self, link, size, key, arrive):
        start = max(self.now, self.free.get(link, 0.0))
        self.free[link] = start + size / LINK_KB_PER_US
        self.events.append((self.free[link] + HOP_US, len(self.events), key, arrive))

    def take(self, event):
        self.events = [e if e is not event else (1e9, e[1], None, None) for e in self.events]
        self.now = max(self.now, event[0]) + 0.03
        self.done.add(event[2])
        event[3]()
        if self.held:
            self.trickle()

    def late(self, key):
        return (key[0] == 2 and key[1] != 0) or (key[0] == 3 and key[2] != 0)

    def release(self):
        self.held = False
        for _, again in self.put_off:
            again()
        self.put_off = []
        self.poll()

    def trickle(self):
        for item in list(self.put_off):
            if self.free.get(item[0], 0.0) <= self.now:
                self.put_off.remove(item)
                item[1]()

    def first(self):
        return min((e for e in self.events if e[2] and not (self.held and self.late(e[2]))), default=(1e9, 0, None, None))

    def poll(self, spent=0.0):
        self.now += spent
        while self.first()[0] <= self.now - 0.5:
            self.take(self.first())

    def until(self, keys):
        while not set(keys) <= self.done:
            self.take(self.first())


class Gather:
    def __init__(self, plan, slot, first_axis, size, place, own, ring_sem, side_sem, send_sem):
        self.plan, self.slot, self.first_axis, self.size, self.place, self.own = plan, slot, first_axis, size, place, own
        self.ring_sem, self.side_sem, self.send_sem = ring_sem, side_sem, send_sem
        self.sent = []
        self.x, self.z, self.h, self.yl, self.c = here()

    def key(self, dx, dz):
        return self.slot, dx % NX, dz % NZ

    def keys(self):
        return [self.key(dx, dz) for dx in range(NX) for dz in range(NZ) if dx or dz]

    def chunk(self, dx, dz):
        return mod(self.x + dx, NX) * NZ + mod(self.z + dz, NZ)

    def send(self, dx, dz, axis, step, granted=False):
        if self.plan.held and self.slot > 1 and axis not in ("side", self.first_axis) and not granted:
            self.plan.put_off.append(((axis, step), lambda: self.send(dx, dz, axis, step, True)))
            return
        ci = self.chunk(dx, dz)
        there = self.place(ci, self.c)
        source = self.own if (dx, dz) == (0, 0) else there
        recv = self.side_sem if axis == "side" else self.ring_sem
        if axis == "side":
            target = ident(self.x, self.z, self.h, self.yl, 1 - self.c)
        elif axis == "x":
            target = ident(mod(self.x + step, NX), self.z, self.h, self.yl, self.c)
        else:
            target = ident(self.x, mod(self.z + step, NZ), self.h, self.yl, self.c)
        copy = pltpu.make_async_remote_copy(
            src_ref=source, dst_ref=there, send_sem=self.send_sem.at[self.slot, len(self.sent)],
            recv_sem=recv.at[self.slot, ci], device_id=target, device_id_type=MESH,
        )
        copy.start()
        self.sent.append(copy)
        if axis != "side":
            seen = (dx - step, dz) if axis == "x" else (dx, dz - step)
            seen = (2 if seen[0] == -2 else seen[0], seen[1])
            self.plan.sent((axis, 1 if step > 0 else -1), self.size * abs(step), self.key(*seen), lambda: self.run(*seen))

    def arrived(self, dx, dz, side=False):
        ci = self.chunk(dx, dz)
        sem = self.side_sem if side else self.ring_sem
        ref = self.place(ci, 1 - self.c if side else self.c)
        pltpu.make_async_remote_copy(
            src_ref=ref, dst_ref=ref, send_sem=self.send_sem.at[self.slot, 0], recv_sem=sem.at[self.slot, ci],
            device_id=ident(self.x, self.z, self.h, self.yl, 1 - self.c), device_id_type=MESH,
        ).wait_recv()

    def begin(self):
        for axis in (self.first_axis, "x" if self.first_axis == "z" else "z"):
            self.send(0, 0, axis, 1)
            self.send(0, 0, axis, -1)
            if self.slot < 2 and axis == self.first_axis:
                self.send(0, 0, axis, 2)
                if axis == "z":
                    self.send(0, 0, axis, -2)
        self.send(0, 0, "side", 0)

    def onward(self, dx, dz):
        s = abs(dz)
        if self.first_axis == "z":
            if dx == 0 and self.slot < 2:
                along = {-2: [("z", 1), ("z", 2)], 2: [("z", -1)]}.get(dz, [])
                return along + [("x", 1), ("x", -1)]
            if dx == 0:
                keep = (dz < 0 and s <= 3) or (dz > 0 and s <= 2)
                return ([("z", 1 if dz < 0 else -1)] if keep else []) + [("x", 1), ("x", -1)]
            first = dz % 8 < 4
            return [("x", 1)] if dx == -1 and first else [("x", -1)] if dx == 1 and not first else []
        if dz == 0:
            return ([("x", 1)] if dx == -1 and self.slot > 1 else []) + [("z", 1), ("z", -1)]
        first = dx in (0, 1)
        if dz < 0:
            return [("z", 1)] if s <= 2 or (s == 3 and first) else []
        return [("z", -1)] if s <= 2 or (s == 3 and not first) else []

    def run(self, dx, dz):
        self.arrived(dx, dz)
        for axis, step in self.onward(dx, dz):
            self.send(dx, dz, axis, step)
        self.send(dx, dz, "side", 0)

    def finish_sides(self):
        for dx in range(NX):
            for dz in range(NZ):
                self.arrived(dx, dz, side=True)

    def finish_sends(self):
        for copy in self.sent:
            copy.wait_send()


def main_kernel(
    q_ref, k_ref, v_ref, seg_ref, freq_ref, w_ref, out_ref,
    kin, vin, krot, win, qin, kall, vall, tags, wall, qa, top, norm, acc, acts, obuf, cown, cpart, cgot,
    ring_sem, side_sem, send_sem, act_send, act_recv, in_send, in_recv, cnt_send, cnt_recv, out_send, out_recv,
):
    x, z, h, yl, c = here()
    y = 2 * h + yl
    ci = x * NZ + z
    far = NCHUNK - 1 - ci
    side = ident(x, z, h, yl, 1 - c)
    swap = ident(x, z, c, yl, h)
    flip_swap = ident(NX - 1 - x, NZ - 1 - z, c, yl, h)
    w_dest = ident(mod(x + plane_shift(y, c), NX), z, lax.rem(x, 2), x // 2, c)
    plane = 2 * yl + h
    away = mod(x - plane, NX)
    from_y = jnp.where(away == 1, jnp.where(c == 0, 1, 3), jnp.where(away == 3, jnp.where(c == 0, 3, 1), away))
    w_source = ident(plane, z, from_y // 2, lax.rem(from_y, 2), c)
    keeps = h == c
    keeps_w = (mod(x + plane_shift(y, c), NX) == x) & (2 * lax.rem(x, 2) + x // 2 == y)

    def along_y(step):
        there = mod(y + step, 4)
        return ident(x, z, there // 2, lax.rem(there, 2), c)

    def heads_at(step):
        there = mod(y + step, 4)
        return 2 * lax.rem(there, 2) + there // 2

    by_z = [ident(x, mod(z + d, NZ), h, yl, c) for d in range(1, NZ)]
    by_xh = [ident(mod(x + d, NX), z, mod(h + e, 2), yl, c) for d in range(NX) for e in range(2) if d or e]
    barrier = pltpu.get_barrier_semaphore()
    always = by_z + by_xh + [along_y(1), along_y(-1), side, flip_swap, swap, w_dest, w_source]
    for peer in always:
        pl.semaphore_signal(barrier, inc=1, device_id=peer, device_id_type=MESH)
    labels = lax.broadcasted_iota(jnp.int32, (BLK, 128), 1)
    own_counts = jnp.sum(jnp.where(seg_ref[...] == labels, 1.0, 0.0), axis=0, keepdims=True)
    cown[...] = jnp.broadcast_to(own_counts, (8, 128)).astype(jnp.int32)
    pl.semaphore_wait(barrier, len(always))

    def remote(slot, source, dest, target, send, recv):
        return pltpu.make_async_remote_copy(
            src_ref=source, dst_ref=dest, send_sem=send.at[slot], recv_sem=recv.at[slot],
            device_id=target, device_id_type=MESH,
        )

    def count_phase(at, source, peers, between):
        copies = [remote(at + i, source, cgot.at[at + i], p, cnt_send, cnt_recv) for i, p in enumerate(peers)]
        for copy in copies:
            copy.start()
        between()
        total = source[...]
        for i, copy in enumerate(copies):
            copy.wait()
            total = total + cgot[at + i]
        return total

    low, high = pl.ds(0, HALF), pl.ds(HALF, HALF)
    moved = {
        "v": (keeps, remote(0, v_ref, vin, swap, in_send, in_recv)),
        "k": (keeps, remote(1, k_ref, kin, swap, in_send, in_recv)),
        "q": (keeps, remote(2, q_ref.at[low], qin.at[low], swap, in_send, in_recv)),
        "w": (keeps_w, remote(3, w_ref, win, w_dest, in_send, in_recv)),
    }
    own_copy = {
        "v": lambda: vin.__setitem__(..., v_ref[...]),
        "k": lambda: kin.__setitem__(..., k_ref[...]),
        "q": lambda: qin.__setitem__((low, slice(None)), q_ref[low, :]),
        "w": lambda: win.__setitem__(..., w_ref[...]),
    }
    upper = remote(4, q_ref.at[high], qin.at[high], flip_swap, in_send, in_recv)

    def start_move(name):
        own, copy = moved[name]
        pl.when(own)(own_copy[name])
        pl.when(jnp.logical_not(own))(copy.start)

    def end_move(name):
        own, copy = moved[name]
        pl.when(jnp.logical_not(own))(copy.wait_recv)

    sems = (ring_sem, side_sem, send_sem)
    plan = Plan()
    a_rows, b_rows = pl.ds(0, WSPLIT), pl.ds(WSPLIT, WROWS - WSPLIT)
    vg = Gather(plan, 0, "z", 48, lambda i, t: vall.at[i, t], vin, *sems)
    kg = Gather(plan, 1, "x", 48, lambda i, t: kall.at[i, t], krot, *sems)
    wa = Gather(plan, 2, "z", WSPLIT / 4, lambda i, t: wall.at[i, t, a_rows], win.at[a_rows], *sems)
    wb = Gather(plan, 3, "x", (WROWS - WSPLIT) / 4, lambda i, t: wall.at[i, t, b_rows], win.at[b_rows], *sems)

    def first_moves():
        start_move("v")
        start_move("k")
        start_move("w")

    def second_moves():
        end_move("v")
        vg.begin()
        vall[ci, c] = vin[...]

    def third_moves():
        start_move("q")
        upper.start()

    cpart[...] = count_phase(0, cown, by_xh, first_moves)
    totals = count_phase(7, cpart, by_z, second_moves)[0:1].astype(jnp.float32)
    third_moves()
    plan.now = 7.0
    lane = lax.broadcasted_iota(jnp.int32, (1, 128), 1)
    ends = totals
    for shift in (1, 2, 4, 8, 16, 32, 64):
        ends = ends + jnp.where(lane >= shift, pltpu.roll(ends, shift, 1), 0.0)
    starts = ends - totals

    def rows_from(first, count):
        return (first + lax.broadcasted_iota(jnp.int32, (count, 128), 0)).astype(jnp.float32)

    def turns(first, count):
        rows = rows_from(first, count)
        start = jnp.max(jnp.where(ends <= rows, ends, 0.0), axis=1, keepdims=True)
        angles = (rows - start) * freq_ref[0:1, :]
        sine = jnp.sin(angles)
        lanes = lax.broadcasted_iota(jnp.int32, (count, 128), 1)
        return jnp.cos(angles), jnp.where(lanes < HEAD_DIM // 2, -sine, sine)

    def rotated(block, cosine, sine):
        wide = block.astype(jnp.float32)
        return (wide * cosine + pltpu.roll(wide, HEAD_DIM // 2, 1) * sine).astype(jnp.bfloat16)

    first_key = ci * CHUNK + c * BLK
    key_cos, key_sin = turns(first_key, BLK)
    end_move("k")
    krot[...] = rotated(kin[...], key_cos, key_sin)
    kg.begin()
    kall[ci, c] = krot[...]
    plan.poll(0.3)
    top[...] = jnp.full(top.shape, BIG, jnp.float32)
    norm[...] = jnp.zeros_like(norm)
    acc[...] = jnp.zeros_like(acc)
    plan.poll(0.4)

    def inside(rows):
        return (rows >= starts) & (rows < ends)

    def tag(i, carry):
        tags[i] = jnp.where(inside(rows_from(i * CHUNK, CHUNK)), 1.0, 0.0).astype(jnp.bfloat16)
        return carry

    lax.fori_loop(0, NCHUNK, tag, 0)
    plan.poll(1.6)
    plan.held = True
    plan.until([vg.key(0, dz) for dz in (1, -1)] + [kg.key(dx, 0) for dx in (1, -1)])
    end_move("w")
    wa.begin()
    wb.begin()
    wall[ci, c] = win[...]
    plan.until(vg.keys() + kg.keys())
    up_cos, up_sin = turns(far * CHUNK + c * BLK + HALF, HALF)
    upper.wait_recv()
    end_move("q")
    for half, (cosine, sine) in enumerate(((key_cos[:HALF], key_sin[:HALF]), (up_cos, up_sin))):
        rows = pl.ds(half * HALF, HALF)
        first_row = ci * CHUNK + c * BLK if half == 0 else far * CHUNK + c * BLK + HALF
        lanes = lax.broadcasted_iota(jnp.int32, (HALF, 128), 1)
        hidden = jnp.logical_not(inside(rows_from(first_row, HALF))) & (lanes < SEGMENTS)
        penalty = jnp.where(hidden, BIG, 0.0).astype(jnp.bfloat16)
        for head in range(GROUP):
            at = pl.ds(head * HALF, HALF)
            qa[half, at, 0:HEAD_DIM] = rotated(qin[rows, head * HEAD_DIM : (head + 1) * HEAD_DIM], cosine, sine)
            qa[half, at, HEAD_DIM : 2 * HEAD_DIM] = penalty
    plan.release()
    kg.finish_sides()
    vg.finish_sides()

    factor = math.log2(math.e) / math.sqrt(HEAD_DIM)

    def attend(half, chunk, mask_from=None):
        keys = jnp.concatenate([kall[chunk].reshape(CHUNK, HEAD_DIM), tags[chunk]], axis=1)
        vals = vall[chunk].reshape(CHUNK, HEAD_DIM)
        size = GROUP * HALF // 2
        tiles = [pl.ds(r, size) for r in range(0, GROUP * HALF, size)]
        olds = [(top[half, r], norm[half, r], acc[half, r]) for r in tiles]

        def scored(r):
            found = lax.dot_general(
                qa[half, r], keys, (((1,), (1,)), ((), ())), preferred_element_type=jnp.float32
            )
            if mask_from is not None:
                row = lax.rem(lax.broadcasted_iota(jnp.int32, found.shape, 0), HALF) + mask_from
                column = chunk * CHUNK + lax.broadcasted_iota(jnp.int32, found.shape, 1)
                found = jnp.where(column <= row, found, BIG)
            return found

        ahead = scored(tiles[0])
        news = []
        for n in range(len(tiles)):
            scores = ahead
            if n + 1 < len(tiles):
                ahead = scored(tiles[n + 1])
            before, total, mix = olds[n]
            peak = jnp.maximum(before, jnp.max(scores, axis=1, keepdims=True))
            fade = jnp.exp2((before - peak) * factor)
            parts = [jnp.exp2((scores[:, i : i + 128] - peak) * factor) for i in range(0, CHUNK, 128)]
            weights = jnp.concatenate([p.astype(jnp.bfloat16) for p in parts], axis=1)
            added = jnp.dot(weights, vals, preferred_element_type=jnp.float32)
            news.append((peak, total * fade + sum(parts[1:], parts[0]), mix * fade + added))
        for r, (a, b, d) in zip(tiles, news):
            top[half, r] = a
            norm[half, r] = b
            acc[half, r] = d

    early = jnp.where(ci < far, 0, 1)
    n_early = jnp.minimum(ci, far)

    def step(i, carry):
        is_early = i < n_early
        attend(jnp.where(is_early, early, 1 - early), jnp.where(is_early, i, i - n_early))
        return carry

    def steps(lo, hi):
        lax.fori_loop(lo, hi, step, 0)
        plan.poll(0.6 * (hi - lo))

    mine = heads_at(0)
    below, above, far_heads = heads_at(-1), heads_at(1), heads_at(2)
    act_copies = []

    def act_start(slot, part, rows, along, key, arrive):
        copy = remote(slot, acts.at[part, rows], acts.at[part, rows], along_y(along), act_send, act_recv)
        copy.start()
        act_copies.append(copy)
        plan.sent(("y", along), 192, key, lambda: arrive(copy))

    def spread(n, half):
        total = jnp.sum(norm[half], axis=1, keepdims=True)
        result = (acc[half] / total).astype(jnp.bfloat16)
        rows = pl.ds(pl.multiple_of(half * HALF, HALF), HALF)
        for head in range(GROUP):
            acts[mine, rows, head * HEAD_DIM : (head + 1) * HEAD_DIM] = result[head * HALF : (head + 1) * HALF]

        def landed(copy):
            copy.wait_recv()

        def onward(copy):
            copy.wait_recv()
            part, along = (below, 1) if n == 0 else (above, -1)
            act_start(3 * n + 2, part, rows, along, ("a", n, 2), landed)

        act_start(3 * n, mine, rows, 1, ("a", n, 0), onward if n == 0 else landed)
        act_start(3 * n + 1, mine, rows, -1, ("a", n, 1), landed if n == 0 else onward)
        plan.poll(0.3)

    attend(0, ci, ci * CHUNK + c * BLK)
    plan.poll(0.7)
    attend(1, far, far * CHUNK + c * BLK + HALF)
    plan.poll(0.7)
    for lo in range(0, 16, 2):
        steps(lo, lo + 2)
    spread(0, early)
    for lo in range(16, 31, 2):
        steps(lo, min(lo + 2, 31))
    spread(1, 1 - early)
    plan.until([("a", n, i) for n in range(2) for i in range(3)])

    given = []
    for dz in ORDER:
        zi = mod(z + dz, NZ)
        plan.until([g.key(dx, dz) for g in (wa, wb) for dx in range(NX) if dx or dz])
        for dx in (0, -1, 1, 2):
            wa.arrived(dx, dz, side=True)
            wb.arrived(dx, dz, side=True)
        total = jnp.zeros((BLK, 256), jnp.float32)
        for kk in range(NX):
            pair = [wall[mod(plane + shift_of(2 * t + kk // 2, kk % 2), NX) * NZ + zi, kk % 2] for t in range(2)]
            total = total + jnp.dot(acts[kk], jnp.concatenate(pair, axis=1), preferred_element_type=jnp.float32)
        block = total.astype(jnp.bfloat16)
        columns = pl.ds(pl.multiple_of(zi * 256, 256), 256)
        lower_copy = remote(zi, obuf.at[zi, low], out_ref.at[low, columns], swap, out_send, out_recv)
        upper_copy = remote(NZ + zi, obuf.at[zi, high], out_ref.at[high, columns], flip_swap, out_send, out_recv)
        given.append((lower_copy, upper_copy))
        obuf[zi] = block
        upper_copy.start()

        @pl.when(keeps)
        def _(columns=columns, block=block):
            out_ref[0:HALF, columns] = block[0:HALF]

        pl.when(jnp.logical_not(keeps))(lower_copy.start)
        plan.poll(1.0)

    for g in (vg, kg, wa, wb):
        g.finish_sends()
    for copy in act_copies:
        copy.wait_send()
    upper.wait_send()
    for own, copy in moved.values():
        pl.when(jnp.logical_not(own))(copy.wait_send)

    for lower_copy, upper_copy in given:
        upper_copy.wait()
        pl.when(jnp.logical_not(keeps))(lower_copy.wait)


def main_call(q, k, v, seg, freq, w):
    rows = GROUP * HALF
    return pl.pallas_call(
        main_kernel,
        out_shape=jax.ShapeDtypeStruct((BLK, NZ * 256), jnp.bfloat16),
        in_specs=[pl.BlockSpec(memory_space=pltpu.VMEM)] * 6,
        out_specs=pl.BlockSpec(memory_space=pltpu.VMEM),
        scratch_shapes=[
            pltpu.VMEM((BLK, HEAD_DIM), jnp.bfloat16),
            pltpu.VMEM((BLK, HEAD_DIM), jnp.bfloat16),
            pltpu.VMEM((BLK, HEAD_DIM), jnp.bfloat16),
            pltpu.VMEM((WROWS, 128), jnp.bfloat16),
            pltpu.VMEM((BLK, GROUP * HEAD_DIM), jnp.bfloat16),
            pltpu.VMEM((NCHUNK, 2, BLK, HEAD_DIM), jnp.bfloat16),
            pltpu.VMEM((NCHUNK, 2, BLK, HEAD_DIM), jnp.bfloat16),
            pltpu.VMEM((NCHUNK, CHUNK, 128), jnp.bfloat16),
            pltpu.VMEM((NCHUNK, 2, WROWS, 128), jnp.bfloat16),
            pltpu.VMEM((2, rows, 2 * HEAD_DIM), jnp.bfloat16),
            pltpu.VMEM((2, rows, 128), jnp.float32),
            pltpu.VMEM((2, rows, 128), jnp.float32),
            pltpu.VMEM((2, rows, HEAD_DIM), jnp.float32),
            pltpu.VMEM((4, BLK, GROUP * HEAD_DIM), jnp.bfloat16),
            pltpu.VMEM((NZ, BLK, 256), jnp.bfloat16),
            pltpu.VMEM((8, 128), jnp.int32),
            pltpu.VMEM((8, 128), jnp.int32),
            pltpu.VMEM((14, 8, 128), jnp.int32),
            pltpu.SemaphoreType.DMA((4, NCHUNK)),
            pltpu.SemaphoreType.DMA((4, NCHUNK)),
            pltpu.SemaphoreType.DMA((4, 64)),
            pltpu.SemaphoreType.DMA((6,)),
            pltpu.SemaphoreType.DMA((6,)),
            pltpu.SemaphoreType.DMA((5,)),
            pltpu.SemaphoreType.DMA((5,)),
            pltpu.SemaphoreType.DMA((14,)),
            pltpu.SemaphoreType.DMA((14,)),
            pltpu.SemaphoreType.DMA((2 * NZ,)),
            pltpu.SemaphoreType.DMA((2 * NZ,)),
        ],
        compiler_params=pltpu.CompilerParams(
            collective_id=2, has_side_effects=True, vmem_limit_bytes=60 * 1024 * 1024
        ),
        name="attend_project",
    )(q, k, v, seg, freq, w)


def local(queries, keys, values, segment_ids, out_weight):
    half_dim = HEAD_DIM // 2
    exponent = jnp.arange(half_dim, dtype=jnp.float32) * (2.0 / HEAD_DIM)
    inverse = jnp.power(jnp.float32(ROPE_BASE), -exponent)
    freq = jnp.broadcast_to(jnp.concatenate([inverse, inverse])[None, :], (8, HEAD_DIM))
    segments = jnp.broadcast_to(segment_ids[:, None], (BLK, 128))
    return main_call(queries, keys, values, segments, freq, out_weight)


def solution(mesh):
    return jax.shard_map(
        local,
        mesh=mesh,
        in_specs=(P("seq", "tp"), P("seq", "tp"), P("seq", "tp"), P("seq"), P("tp", "seq")),
        out_specs=P("seq", "tp"),
        check_vma=False,
    )
```
